256 devices in a mesh: dp: 8 (over x, core), mp: 32 (over y, z).
Axes of the slice: x: 4, y: 4, z: 8, core: 2. Of those that a mesh axis runs over, the one named last changes fastest.
Arguments:
- gradients: bfloat16 [8, 4096, 16384], P('dp', None, 'mp'), may hold values from -40 to 40
- owner_table: int32 [512], replicated, may hold values from 0 to 31, as said below
Outputs:
- root_stacks: float32 [32, 24, 512, 512], P('mp', 'dp')
- slab_roots: float32 [16, 512, 16384], P(None, 'dp', 'mp')
The draws below stay inside these ranges and needn't reach their ends.
Inputs may be any that keep to these rules, and one draw needn't show every extreme that they name: `owner_table`: statistic m * 16 + i belongs to column slab m. No owner is named by more than 24 statistics and some owner by exactly 24; among the 16 statistics of one column slab no owner is named more than 1 times, and some slab names some owner exactly 1 times.
All inputs are finite; a program needn't handle non-finite values.
Results may differ from the reference program's by a relative error of at most 0.0017.
Values may be sent and summed in bfloat16 or wider, within the bound.
No kernel may reach another device: no remote copies, remote signals or barrier semaphores. Data moves between devices by JAX's collectives and lax.ppermute only.
A program may use at most 320 MiB of HBM per device.

```python
import jax
import jax.numpy as jnp
from jax import lax

BLOCK = 512
ROWS = 4096
ITERS = 3
CAP = 24
COLS = 16384
ROW_BLOCKS = 8
PER_SLAB = 16
STATS = 512
N_DP = 8
N_MP = 32


def draw_gradients(key, part):
    noise_key = jax.random.fold_in(key, 0)
    shape_full = (N_DP, ROWS, COLS)
    values = jax.random.normal(noise_key, shape_full, jnp.float32)
    shard_scale = 1.0 + 2.0 * jnp.arange(N_DP, dtype=jnp.float32) / max(N_DP - 1, 1)
    values = values * shard_scale[:, None, None] * BLOCK ** (-0.5)
    return values.astype(jnp.bfloat16)


def draw_owner_table(key, part):
    per_slab_count = 2 * (ROWS // BLOCK)
    order_key, amount_key = jax.random.split(key)
    owner_order = jax.random.permutation(order_key, N_MP)
    half_count = N_MP // 2
    amount = jax.random.randint(amount_key, (half_count,), 0, CAP - per_slab_count + 1)
    amount = amount.at[0].set(CAP - per_slab_count)
    ranked = (per_slab_count + jnp.concatenate([amount, -amount])).astype(jnp.int32)
    owner_loads = jnp.zeros((N_MP,), jnp.int32).at[owner_order].set(ranked)
    load_ends = jnp.cumsum(owner_loads)
    positions = jnp.arange(N_MP * per_slab_count, dtype=jnp.int32)
    sorted_owner = jnp.sum((positions[:, None] >= load_ends[None, :]).astype(jnp.int32), axis=1)
    slab_index = positions // per_slab_count
    within_slab = positions % per_slab_count
    return sorted_owner[within_slab * N_MP + slab_index].astype(jnp.int32)


def setup_inputs(seed: int = 0) -> dict:
    keys = jax.random.split(jax.random.key(seed), 3)
    gradients = draw_gradients(jax.random.fold_in(keys[2], 71), 0)
    owner_table = draw_owner_table(jax.random.fold_in(keys[2], 71), 0)
    return dict(gradients=gradients, owner_table=owner_table)


def batched(first, second):
    return jnp.einsum('kab,kbc->kac', first, second, precision=lax.Precision.HIGHEST)

def newton_roots(statistics, iterations):
    matrix_size = statistics.shape[-1]
    identity = jnp.eye(matrix_size, dtype=jnp.float32)
    diagonal_mean = lax.optimization_barrier(jnp.mean(jnp.diagonal(statistics, axis1=1, axis2=2), axis=1))
    damped = statistics + 0.1 * diagonal_mean[:, None, None] * identity[None]
    mean_square = lax.optimization_barrier(jnp.mean(damped * damped, axis=(1, 2)))
    norm_scale = matrix_size * jnp.sqrt(mean_square + 1e-06)
    matrix = damped / norm_scale[:, None, None]
    root_scale = norm_scale ** (-0.25)
    current = matrix
    for iteration in range(iterations):
        factor = (5.0 * identity - matrix) * 0.25
        if iteration == 0:
            current = factor * root_scale[:, None, None]
        else:
            current = batched(current, factor)
        if iteration + 1 < iterations:
            square = batched(factor, factor)
            matrix = batched(square, batched(square, matrix))
    return current

def reference(gradients, owner_table):

    def slab_work(column):
        first_column = (column * BLOCK).astype(jnp.int32)
        column_slab = lax.dynamic_slice_in_dim(gradients, first_column, BLOCK, 2).astype(jnp.float32)
        blocks = column_slab.reshape(N_DP, ROW_BLOCKS, BLOCK, BLOCK)
        left_gram = jnp.einsum('drab,drcb->drac', blocks, blocks)
        right_gram = jnp.einsum('drab,drac->drbc', blocks, blocks)
        partial_value = jnp.stack([left_gram, right_gram], axis=2).reshape(N_DP, PER_SLAB, BLOCK, BLOCK)
        rounded = lax.optimization_barrier(partial_value.astype(jnp.bfloat16)).astype(jnp.float32)
        statistics = lax.optimization_barrier(jnp.sum(rounded, axis=0)) * (1.0 / N_DP)
        return newton_roots(statistics, ITERS)
    all_roots = lax.map(slab_work, jnp.arange(N_MP, dtype=jnp.int32))
    slab_roots = jnp.transpose(all_roots, (1, 2, 0, 3)).reshape(PER_SLAB, BLOCK, COLS)
    owner_ids = jnp.arange(N_MP, dtype=jnp.int32)
    onehot = (owner_table[:, None] == owner_ids[None, :]).astype(jnp.int32)
    slot_number = lax.optimization_barrier(jnp.sum((jnp.cumsum(onehot, axis=0) - onehot) * onehot, axis=1)).astype(jnp.int32)
    flat_roots = all_roots.reshape(STATS, BLOCK, BLOCK)
    root_stacks = jnp.zeros((N_MP, CAP, BLOCK, BLOCK), jnp.float32).at[owner_table, slot_number].set(flat_roots)
    return (root_stacks, slab_roots)
```

```python
import functools

import jax
import jax.numpy as jnp
from jax import lax
from jax.experimental import pallas as pl
from jax.experimental.pallas import tpu as pltpu
from jax.sharding import PartitionSpec as P

CAP = 24
BLOCK = 512
TILE = 128
UPPER = [(0, 0), (0, 1), (0, 2), (0, 3), (1, 1), (1, 2), (1, 3), (2, 2), (2, 3), (3, 3)]
HALF = len(UPPER) // 2
HALF_ROWS = HALF * TILE
PACKED_ROWS = len(UPPER) * TILE
ALPHA_ORDER = (1, 2, 0, 3)
BETA_ORDER = (3, 2, 0, 1)
INTERPRET = False
F32 = jnp.float32
BF16 = jnp.bfloat16


def rows_of(block):
    return slice(block * TILE, (block + 1) * TILE)


def dot(first, second, dims=((1,), (0,))):
    return lax.dot_general(first, second, (dims, ((), ())), preferred_element_type=F32)


def gram_kernel(place_ref, block_ref, alpha_ref, beta_ref):
    block = block_ref[0]
    half = BLOCK // 2
    for side in range(2):
        dims = ((1,), (1,)) if side == 0 else ((0,), (0,))
        low = block[:half] if side == 0 else block[:, :half]
        high = block[half:] if side == 0 else block[:, half:]
        top = dot(low, block, dims).astype(BF16)
        bottom = dot(high, high, dims).astype(BF16)
        for index, (row, column) in enumerate(UPPER):
            if row < 2:
                piece = top[rows_of(row), rows_of(column)]
            else:
                piece = bottom[rows_of(row - 2), rows_of(column - 2)]
            target = alpha_ref if index < HALF else beta_ref
            target[0, side, rows_of(index % HALF), :] = piece


def gram_blocks(blocks, place, core_bit):
    def which(order):
        def index_map(step, place_ref):
            return (order(step), 0, 0, 0)

        return index_map

    alpha_slot = [ALPHA_ORDER.index(t) for t in range(4)]
    beta_slot = [BETA_ORDER.index(t) for t in range(4)]

    def table(slots):
        def order(step):
            result = slots[3]
            for t in range(3):
                result = jnp.where(step == t, slots[t], result)
            return result

        return order

    shape = jax.ShapeDtypeStruct((4, 2, HALF_ROWS, TILE), BF16)
    grid_spec = pltpu.PrefetchScalarGridSpec(
        num_scalar_prefetch=1,
        grid=(4,),
        in_specs=[
            pl.BlockSpec(
                (1, BLOCK, BLOCK),
                lambda step, place_ref: (place_ref[0] ^ (2 * step + core_bit), 0, 0),
            )
        ],
        out_specs=[
            pl.BlockSpec((1, 2, HALF_ROWS, TILE), which(table(alpha_slot))),
            pl.BlockSpec((1, 2, HALF_ROWS, TILE), which(table(beta_slot))),
        ],
    )
    return pl.pallas_call(
        gram_kernel,
        out_shape=(shape, shape),
        grid_spec=grid_spec,
        interpret=INTERPRET,
        name="gram" + str(core_bit),
        cost_estimate=pl.CostEstimate(
            flops=4 * 2 * 3 * BLOCK**3 // 2, bytes_accessed=5 * 2**20, transcendentals=0
        ),
    )(place, blocks)


def iota(shape, axis):
    return lax.broadcasted_iota(jnp.int32, shape, axis)


def total(value):
    return jnp.sum(jnp.sum(value, axis=0, keepdims=True), axis=1, keepdims=True)


def power_four(matrix, small, product):
    square = dot(small, small)
    part = (square * 0.0625 - 0.625 * matrix).astype(BF16)
    once = 1.5625 * matrix + dot(part, small)
    return 1.5625 * once + dot(part, once.astype(BF16))


def newton_kernel(parts, data_count, refs, rows_ref, packed_ref, stat_ref):
    row_ids = iota((BLOCK, BLOCK), 0)
    column_ids = iota((BLOCK, BLOCK), 1)
    on_diagonal = row_ids == column_ids
    spare = (row_ids % 64 == 1) & (column_ids == row_ids - 1)
    for stat in range(2):
        for index, (row, column) in enumerate(UPPER):
            piece = None
            for ref in refs[parts * (index // HALF) : parts * (index // HALF) + parts]:
                term = ref[0, stat, rows_of(index % HALF), :].astype(F32)
                piece = term if piece is None else piece + term
            stat_ref[rows_of(row), rows_of(column)] = piece
            if row != column:
                stat_ref[rows_of(column), rows_of(row)] = piece.T
        statistic = stat_ref[...] * (1.0 / data_count)
        diagonal_mean = total(jnp.where(on_diagonal, statistic, 0.0)) * (1.0 / BLOCK)
        damped = statistic + jnp.where(on_diagonal, 0.1 * diagonal_mean, 0.0)
        mean_square = total(damped * damped) * (1.0 / BLOCK**2)
        norm_scale = BLOCK * jnp.sqrt(mean_square + 1e-06)
        root_scale = lax.rsqrt(jnp.sqrt(norm_scale))
        first = damped / norm_scale
        first_small = first.astype(BF16)
        second = power_four(first, first_small, None)
        second_small = second.astype(BF16)
        pair = dot(first_small, second_small) * 0.0625 - 0.3125 * (first + second)
        third = power_four(second, second_small, None)
        rest = 1.25 * pair - 0.390625 * third - 0.25 * dot(pair.astype(BF16), third.astype(BF16))
        rest = rest * root_scale
        rest_mean = total(jnp.where(on_diagonal, rest, 0.0)) * (1.0 / BLOCK)
        identity_part = 1.953125 * root_scale
        center = (identity_part + rest_mean).astype(BF16).astype(F32)
        rest = rest + jnp.where(on_diagonal, identity_part - center, 0.0)
        sent = jnp.where(spare, center, rest).astype(BF16)
        for device in range(8):
            rows_ref[device, stat] = sent[device * 64 : (device + 1) * 64]
        for index, (row, column) in enumerate(UPPER):
            piece = sent[rows_of(row), rows_of(column)]
            start = index * TILE
            while start < (index + 1) * TILE:
                device = start // CHUNK
                stop = min((index + 1) * TILE, (device + 1) * CHUNK)
                packed_ref[device, stat, start - device * CHUNK : stop - device * CHUNK, :] = piece[
                    start - index * TILE : stop - index * TILE
                ]
                start = stop


CHUNK = PACKED_ROWS // 8


def newton(alpha, beta, data_count):
    parts = len(alpha)

    def body(*refs):
        newton_kernel(parts, data_count, refs[: 2 * parts], *refs[2 * parts :])

    def spec(place):
        return pl.BlockSpec((1, 2, HALF_ROWS, TILE), lambda step: (place, 0, 0, 0))

    return pl.pallas_call(
        body,
        grid=(1,),
        in_specs=[spec(place) for _, place in alpha + beta],
        out_specs=[
            pl.BlockSpec((8, 2, 64, BLOCK), lambda step: (0, 0, 0, 0)),
            pl.BlockSpec((8, 2, CHUNK, TILE), lambda step: (0, 0, 0, 0)),
        ],
        out_shape=(
            jax.ShapeDtypeStruct((8, 2, 64, BLOCK), BF16),
            jax.ShapeDtypeStruct((8, 2, CHUNK, TILE), BF16),
        ),
        scratch_shapes=[pltpu.VMEM((BLOCK, BLOCK), F32)],
        interpret=INTERPRET,
        name="newton",
        cost_estimate=pl.CostEstimate(
            flops=2 * 8 * 2 * BLOCK**3, bytes_accessed=6 * 2**20, transcendentals=0
        ),
    )(*[array for array, _ in alpha + beta])


def pick_kernel(index_ref, source_ref, out_ref):
    def step(place, carry):
        out_ref[place] = source_ref[index_ref[place]]
        return carry

    lax.fori_loop(0, out_ref.shape[0], step, 0)


def pick(source, index, name):
    count = index.shape[0]
    return pl.pallas_call(
        pick_kernel,
        out_shape=jax.ShapeDtypeStruct((count,) + source.shape[1:], source.dtype),
        in_specs=[
            pl.BlockSpec(memory_space=pltpu.SMEM),
            pl.BlockSpec(memory_space=pltpu.VMEM),
        ],
        out_specs=pl.BlockSpec(memory_space=pltpu.VMEM),
        interpret=INTERPRET,
        name=name,
        cost_estimate=pl.CostEstimate(flops=2 * 10**6, bytes_accessed=2 * 2**20, transcendentals=0),
    )(index, source)


def make_plan(owner_table, model_index, model_count, per_slab):
    owner_ids = jnp.arange(model_count, dtype=jnp.int32)
    mine = lax.dynamic_slice_in_dim(owner_table, model_index * per_slab, per_slab)
    local_ids = jnp.arange(per_slab, dtype=jnp.int32)
    send_index = jnp.sum(
        jnp.where(mine[None, :] == owner_ids[:, None], local_ids[None, :], 0), axis=1
    )
    named = jnp.sum(
        (owner_table.reshape(model_count, per_slab) == model_index).astype(jnp.int32), axis=1
    )
    rank = jnp.sum(
        jnp.where(owner_ids[None, :] < owner_ids[:, None], named[None, :], 0), axis=1
    )
    slot_ids = jnp.arange(CAP, dtype=jnp.int32)
    match = (rank[None, :] == slot_ids[:, None]) & (named[None, :] > 0)
    slot_index = jnp.sum(jnp.where(match, owner_ids[None, :], 0), axis=1)
    return send_index, slot_index, jnp.sum(named)


def unpack_kernel(valid_ref, source_ref, out_ref, stack_ref):
    slot = pl.program_id(0)
    keep = valid_ref[slot] > 0

    @pl.when(keep)
    def _():
        for device in range(8):
            stack_ref[device * CHUNK : (device + 1) * CHUNK, :] = source_ref[device, 0].astype(F32)
        center = stack_ref[1:2, 0:1]
        row_ids = iota((TILE, TILE), 0)
        column_ids = iota((TILE, TILE), 1)
        spare = (row_ids % 64 == 1) & (column_ids == row_ids - 1)
        for index, (row, column) in enumerate(UPPER):
            piece = stack_ref[rows_of(index), :]
            if row == column:
                piece = jnp.where(spare, piece.T, piece)
                piece = jnp.where(row_ids == column_ids, piece + center, piece)
            else:
                out_ref[0, rows_of(column), rows_of(row)] = piece.T
            out_ref[0, rows_of(row), rows_of(column)] = piece

    @pl.when(jnp.logical_not(keep))
    def _():
        out_ref[...] = jnp.zeros_like(out_ref)


def unpack(source, valid):
    slots = source.shape[1]
    return pl.pallas_call(
        unpack_kernel,
        out_shape=jax.ShapeDtypeStruct((slots, BLOCK, BLOCK), F32),
        grid_spec=pltpu.PrefetchScalarGridSpec(
            num_scalar_prefetch=1,
            grid=(slots,),
            in_specs=[pl.BlockSpec((8, 1, CHUNK, TILE), lambda slot, valid_ref: (0, slot, 0, 0))],
            out_specs=pl.BlockSpec((1, BLOCK, BLOCK), lambda slot, valid_ref: (slot, 0, 0)),
            scratch_shapes=[pltpu.VMEM((PACKED_ROWS, TILE), F32)],
        ),
        interpret=INTERPRET,
        name="unpack",
        cost_estimate=pl.CostEstimate(flops=2 * 10**6, bytes_accessed=4 * 2**20, transcendentals=0),
    )(valid, source)


def finish_rows(rows, data_index):
    stats, count, width = rows.shape
    first = data_index * count
    columns = jnp.arange(width, dtype=jnp.int32)
    center = jnp.sum(jnp.where(columns == first, rows[:, 1, :].astype(F32), 0.0), axis=1)
    mirrored = jnp.sum(jnp.where(columns == first + 1, rows[:, 0, :].astype(F32), 0.0), axis=1)
    row_ids = iota((count, width), 0)
    column_ids = iota((count, width), 1) - first
    spare = (row_ids == 1) & (column_ids == 0)
    value = jnp.where(spare[None], mirrored[:, None, None], rows.astype(F32))
    return value + jnp.where((row_ids == column_ids)[None], center[:, None, None], 0.0)


def add(first, second):
    return (first.astype(F32) + second.astype(F32)).astype(BF16)


def exchange(value, bits, data_count):
    return lax.ppermute(value, "dp", [(d, d ^ bits) for d in range(data_count)])


def on_device(gradients, owner_table):
    data_count = lax.axis_size("dp")
    model_count = lax.axis_size("mp")
    data_index = lax.axis_index("dp")
    model_index = lax.axis_index("mp")
    row_blocks = gradients.shape[1] // BLOCK
    per_slab = 2 * row_blocks
    blocks = gradients[0].reshape(row_blocks, BLOCK, BLOCK)
    place = data_index.astype(jnp.int32).reshape(1)

    away_alpha, away_beta = gram_blocks(blocks, place, 1)
    got_alpha = exchange(away_alpha, 1, data_count)
    got_beta = exchange(away_beta, 1, data_count)
    own_alpha, own_beta = gram_blocks(blocks, place, 0)

    step_alpha = exchange(add(own_alpha[:2], got_alpha[:2]), 2, data_count)
    step_beta = exchange(add(own_beta[:2], got_beta[:2]), 6, data_count)

    def second(own, got, step, bits):
        value = own[3:4].astype(F32) + got[3:4].astype(F32) + step[1:2].astype(F32)
        return exchange(value.astype(BF16), bits, data_count)

    last_alpha = second(own_alpha, got_alpha, step_alpha, 6)
    last_beta = second(own_beta, got_beta, step_beta, 2)

    rows, packed = newton(
        [(own_alpha, 2), (got_alpha, 2), (step_alpha, 0), (last_alpha, 0)],
        [(own_beta, 2), (got_beta, 2), (step_beta, 0), (last_beta, 0)],
        data_count,
    )

    send_index, slot_index, load = make_plan(owner_table, model_index, model_count, per_slab)

    pieces = lax.all_to_all(packed, "dp", split_axis=0, concat_axis=0, tiled=True)
    row_pieces = lax.all_to_all(rows, "dp", split_axis=0, concat_axis=0, tiled=True)
    outgoing = pick(pieces.reshape(per_slab, CHUNK, TILE), send_index, "send_pick")
    incoming = lax.all_to_all(outgoing, "mp", split_axis=0, concat_axis=0, tiled=True)
    slab_roots = finish_rows(row_pieces.reshape(per_slab, BLOCK // data_count, BLOCK), data_index)
    slots = pick(incoming, slot_index, "slot_pick")
    stacked = lax.all_to_all(slots, "dp", split_axis=0, concat_axis=0, tiled=True)
    own_slots = CAP // data_count
    slot_ids = data_index * own_slots + jnp.arange(own_slots, dtype=jnp.int32)
    valid = (slot_ids < load).astype(jnp.int32)
    root_stacks = unpack(stacked.reshape(data_count, own_slots, CHUNK, TILE), valid)
    return (root_stacks[None], slab_roots)


def solution(mesh):
    placed = (P("dp", None, "mp"), P())
    return jax.shard_map(
        on_device,
        mesh=mesh,
        in_specs=placed,
        out_specs=(P("mp", "dp", None, None), P(None, "dp", "mp")),
        check_vma=False,
    )
```

```python
import jax
import jax.numpy as jnp
from jax import lax
from jax.experimental import pallas as pl
from jax.experimental.pallas import tpu as pltpu
from jax.sharding import PartitionSpec as P

CAP = 24
BLOCK = 512
TILE = 128
DEVICES = 8
UPPER = [(0, 0), (0, 1), (0, 2), (0, 3), (1, 1), (1, 2), (1, 3), (2, 2), (2, 3), (3, 3)]
PACKED_ROWS = len(UPPER) * TILE
CHUNK = PACKED_ROWS // DEVICES
PIECE = CHUNK // 2
ROWS = BLOCK // DEVICES
ORDERS = ((1, 2, 0, 3), (3, 2, 0, 1))
FIRST_BITS = (2, 6)
SECOND_BITS = (6, 2)
INTERPRET = False
F32 = jnp.float32
BF16 = jnp.bfloat16


def rows_of(block):
    return slice(block * TILE, (block + 1) * TILE)


def dot(first, second, dims=((1,), (0,))):
    return lax.dot_general(first, second, (dims, ((), ())), preferred_element_type=F32)


def iota(shape, axis):
    return lax.broadcasted_iota(jnp.int32, shape, axis)


def whole(memory_space=pltpu.VMEM):
    return pl.BlockSpec(memory_space=memory_space)


def cost(flops, moved):
    return pl.CostEstimate(flops=int(flops), bytes_accessed=int(moved), transcendentals=0)


def gram_kernel(device_ref, block_ref, own_ref, away_ref, stack_ref):
    block = block_ref[0]
    half = BLOCK // 2
    core = device_ref[0] & 1
    along = device_ref[0] >> 1
    for side in range(2):
        dims = ((1,), (1,)) if side == 0 else ((0,), (0,))
        low = block[:half] if side == 0 else block[:, :half]
        high = block[half:] if side == 0 else block[:, half:]
        right = dot(block, high, dims).astype(BF16)
        corner = dot(low, low, dims).astype(BF16)
        for index, (row, column) in enumerate(UPPER):
            if column >= 2:
                piece = right[rows_of(row), rows_of(column - 2)]
            else:
                piece = corner[rows_of(row), rows_of(column)]
            stack_ref[rows_of(index)] = piece
        for chip in range(4):
            offset = chip ^ along
            for part in range(2):
                place = jnp.int32(0)
                for spot, value in enumerate(ORDERS[part]):
                    place = jnp.where(offset == value, spot, place)
                even = stack_ref[pl.ds((4 * chip + part) * PIECE, PIECE)]
                odd = stack_ref[pl.ds((4 * chip + 2 + part) * PIECE, PIECE)]
                own_ref[part, place, side] = jnp.where(core == 0, even, odd)
                away_ref[part, place, side] = jnp.where(core == 0, odd, even)


def gram_blocks(blocks, device, first, count):
    shape = jax.ShapeDtypeStruct((2, 4, 2 * count, PIECE, TILE), BF16)
    out_spec = pl.BlockSpec((2, 4, 2, PIECE, TILE), lambda step, device_ref: (0, 0, step, 0, 0))
    return pl.pallas_call(
        gram_kernel,
        out_shape=(shape, shape),
        grid_spec=pltpu.PrefetchScalarGridSpec(
            num_scalar_prefetch=1,
            grid=(count,),
            in_specs=[
                pl.BlockSpec((1, BLOCK, BLOCK), lambda step, device_ref: (first + step, 0, 0))
            ],
            out_specs=[out_spec, out_spec],
            scratch_shapes=[pltpu.VMEM((PACKED_ROWS, TILE), BF16)],
        ),
        interpret=INTERPRET,
        name="gram" + str(first),
        cost_estimate=cost(3 * count * BLOCK**3, count * 5 * 2**18),
    )(device, blocks)


def sum_kernel(device_ref, send_ref, *refs):
    mine_ref = refs[-1]
    outgoing_ref = refs[12]
    home_refs = refs[13:-1]
    count = refs[0].shape[2]
    for group in range(2):
        own_ref, got_ref, *rest = refs[6 * group : 6 * group + 6]
        for part in range(2):
            step_ref, last_ref = rest[2 * part : 2 * part + 2]
            value = own_ref[part, 0].astype(F32) + got_ref[part, 0].astype(F32)
            value = value + step_ref[0].astype(F32) + last_ref[0].astype(F32)
            mine_ref[group * count : (group + 1) * count, part * PIECE : (part + 1) * PIECE] = (
                value.astype(BF16)
            )

    def send(place, carry):
        outgoing_ref[place] = mine_ref[send_ref[place]]
        return carry

    lax.fori_loop(0, outgoing_ref.shape[0], send, 0)
    for bits, home_ref in enumerate(home_refs):
        home = device_ref[0] ^ bits
        for stat in range(2):
            home_ref[stat] = mine_ref[2 * home + stat]


def sum_and_send(device, send_index, groups):
    operands, specs = [], []
    count = groups[0][0].shape[2]
    for own, got, parts in groups:
        for array in (own, got):
            operands.append(array)
            specs.append(pl.BlockSpec((2, 1, count, PIECE, TILE), lambda step: (0, 2, 0, 0, 0)))
        for step, last in parts:
            for array in (step, last):
                operands.append(array)
                specs.append(pl.BlockSpec((1, count, PIECE, TILE), lambda step: (0, 0, 0, 0)))
    owners = send_index.shape[0]
    home = jax.ShapeDtypeStruct((2, CHUNK, TILE), BF16)
    return pl.pallas_call(
        sum_kernel,
        grid=(1,),
        in_specs=[whole(pltpu.SMEM), whole(pltpu.SMEM)] + specs,
        out_specs=[whole()] * (1 + DEVICES),
        out_shape=[jax.ShapeDtypeStruct((owners, CHUNK, TILE), BF16)] + [home] * DEVICES,
        scratch_shapes=[pltpu.VMEM((2 * count, CHUNK, TILE), BF16)],
        interpret=INTERPRET,
        name="sum_and_send",
        cost_estimate=cost(2**21, 2**22),
    )(device, send_index, *operands)


def slot_kernel(device_ref, index_ref, source_ref, *slot_refs):
    slots = slot_refs[0].shape[0]
    for bits, slot_ref in enumerate(slot_refs):
        home = device_ref[0] ^ bits
        for slot in range(slots):
            slot_ref[slot] = source_ref[index_ref[slots * home + slot]]


def slot_pick(device, slot_index, incoming):
    slots = CAP // DEVICES
    return pl.pallas_call(
        slot_kernel,
        in_specs=[whole(pltpu.SMEM), whole(pltpu.SMEM), whole()],
        out_specs=[whole()] * DEVICES,
        out_shape=[jax.ShapeDtypeStruct((slots, CHUNK, TILE), BF16)] * DEVICES,
        interpret=INTERPRET,
        name="slot_pick",
        cost_estimate=cost(2**21, 2**22),
    )(device, slot_index, incoming)


def total(value):
    return jnp.sum(jnp.sum(value, axis=0, keepdims=True), axis=1, keepdims=True)


def power_four(matrix, small):
    square = dot(small, small)
    part = (square * 0.0625 - 0.625 * matrix).astype(BF16)
    once = 1.5625 * matrix + dot(part, small)
    return 1.5625 * once + dot(part, once.astype(BF16))


def root_of(device_ref, refs, stat, data_count, stack_ref, stat_ref):
    for bits, ref in enumerate(refs):
        stack_ref[device_ref[0] ^ bits] = ref[stat].astype(F32)
    for index, (row, column) in enumerate(UPPER):
        start, stop = index * TILE, (index + 1) * TILE
        while start < stop:
            chunk = start // CHUNK
            end = min(stop, (chunk + 1) * CHUNK)
            piece = stack_ref[chunk, start - chunk * CHUNK : end - chunk * CHUNK]
            base = row * TILE + start - index * TILE
            stat_ref[base : base + end - start, rows_of(column)] = piece
            start = end
        if row != column:
            stat_ref[rows_of(column), rows_of(row)] = stat_ref[rows_of(row), rows_of(column)].T
    on_diagonal = iota((BLOCK, BLOCK), 0) == iota((BLOCK, BLOCK), 1)
    statistic = stat_ref[...] * (1.0 / data_count)
    diagonal_mean = total(jnp.where(on_diagonal, statistic, 0.0)) * (1.0 / BLOCK)
    damped = statistic + jnp.where(on_diagonal, 0.1 * diagonal_mean, 0.0)
    mean_square = total(damped * damped) * (1.0 / BLOCK**2)
    norm_scale = BLOCK * jnp.sqrt(mean_square + 1e-06)
    root_scale = lax.rsqrt(jnp.sqrt(norm_scale))
    first = damped * (1.0 / norm_scale)
    first_small = first.astype(BF16)
    second = power_four(first, first_small)
    second_small = second.astype(BF16)
    pair = dot(first_small, second_small) * 0.0625 - 0.3125 * (first + second)
    third = power_four(second, second_small)
    rest = 1.25 * pair - 0.390625 * third - 0.25 * dot(pair.astype(BF16), third.astype(BF16))
    return rest * root_scale, 1.953125 * root_scale, on_diagonal


def home_kernel(data_count, device_ref, *refs):
    sources, (stack_ref, stat_ref) = refs[:DEVICES], refs[-2:]
    row_refs = refs[DEVICES : 2 * DEVICES]
    rows_ref = refs[-3]
    row_ids = iota((BLOCK, BLOCK), 0)
    spare = (row_ids % ROWS == 1) & (iota((BLOCK, BLOCK), 1) == row_ids - 1)
    for stat in range(2):
        rest, identity_part, on_diagonal = root_of(
            device_ref, sources, stat, data_count, stack_ref, stat_ref
        )
        rest_mean = total(jnp.where(on_diagonal, rest, 0.0)) * (1.0 / BLOCK)
        center = (identity_part + rest_mean).astype(BF16).astype(F32)
        rest = rest + jnp.where(on_diagonal, identity_part - center, 0.0)
        sent = jnp.where(spare, center, rest).astype(BF16)
        for device in range(DEVICES):
            rows_ref[device] = sent[device * ROWS : (device + 1) * ROWS]
        for bits, row_ref in enumerate(row_refs):
            row_ref[stat] = rows_ref[device_ref[0] ^ bits]


def home_roots(device, sources, data_count):
    return pl.pallas_call(
        lambda *refs: home_kernel(data_count, *refs),
        in_specs=[whole(pltpu.SMEM)] + [whole()] * DEVICES,
        out_specs=[whole()] * DEVICES,
        out_shape=[jax.ShapeDtypeStruct((2, ROWS, BLOCK), BF16)] * DEVICES,
        scratch_shapes=[
            pltpu.VMEM((DEVICES, ROWS, BLOCK), BF16),
            pltpu.VMEM((DEVICES, CHUNK, TILE), F32),
            pltpu.VMEM((BLOCK, BLOCK), F32),
        ],
        interpret=INTERPRET,
        name="home_roots",
        cost_estimate=cost(2 * 8 * 2 * BLOCK**3, 2**22),
    )(device, *sources)


def owner_roots(device, load, sources, data_count):
    slots = sources[0].shape[0]

    def body(device_ref, load_ref, *refs):
        sources, (out_ref, stack_ref, stat_ref) = refs[:DEVICES], refs[DEVICES:]
        slot = pl.program_id(0)
        keep = slots * device_ref[0] + slot < load_ref[0]

        @pl.when(keep)
        def _():
            rest, identity_part, on_diagonal = root_of(
                device_ref, sources, 0, data_count, stack_ref, stat_ref
            )
            out_ref[0] = rest + jnp.where(on_diagonal, identity_part, 0.0)

        @pl.when(jnp.logical_not(keep))
        def _():
            out_ref[...] = jnp.zeros_like(out_ref)

    return pl.pallas_call(
        body,
        grid=(slots,),
        in_specs=[whole(pltpu.SMEM), whole(pltpu.SMEM)]
        + [pl.BlockSpec((1, CHUNK, TILE), lambda slot: (slot, 0, 0))] * DEVICES,
        out_specs=pl.BlockSpec((1, BLOCK, BLOCK), lambda slot: (slot, 0, 0)),
        out_shape=jax.ShapeDtypeStruct((slots, BLOCK, BLOCK), F32),
        scratch_shapes=[
            pltpu.VMEM((DEVICES, CHUNK, TILE), F32),
            pltpu.VMEM((BLOCK, BLOCK), F32),
        ],
        interpret=INTERPRET,
        name="owner_roots",
        cost_estimate=cost(3 * 8 * 2 * BLOCK**3, 2**22),
    )(device, load, *sources)


def finish_kernel(device_ref, *refs):
    out_ref = refs[-1]
    first = device_ref[0] * ROWS
    row_ids = iota((ROWS, BLOCK), 0)
    column_ids = iota((ROWS, BLOCK), 1) - first
    spare = (row_ids == 1) & (column_ids == 0)
    mirror = (row_ids == 0) & (column_ids == 1)
    on_diagonal = row_ids == column_ids
    for bits, ref in enumerate(refs[:-1]):
        home = device_ref[0] ^ bits
        for stat in range(2):
            value = ref[stat].astype(F32)
            center = total(jnp.where(spare[:8], value[:8], 0.0))
            mirrored = total(jnp.where(mirror[:8], value[:8], 0.0))
            value = jnp.where(spare, mirrored, value)
            out_ref[2 * home + stat] = value + jnp.where(on_diagonal, center, 0.0)


def finish_rows(device, rows):
    return pl.pallas_call(
        finish_kernel,
        in_specs=[whole(pltpu.SMEM)] + [whole()] * DEVICES,
        out_specs=whole(),
        out_shape=jax.ShapeDtypeStruct((2 * DEVICES, ROWS, BLOCK), F32),
        interpret=INTERPRET,
        name="finish_rows",
        cost_estimate=cost(2**21, 2**22),
    )(device, *rows)


def make_plan(owner_table, model_index, model_count, per_slab):
    owner_ids = jnp.arange(model_count, dtype=jnp.int32)
    mine = lax.dynamic_slice_in_dim(owner_table, model_index * per_slab, per_slab)
    local_ids = jnp.arange(per_slab, dtype=jnp.int32)
    send_index = jnp.sum(
        jnp.where(mine[None, :] == owner_ids[:, None], local_ids[None, :], 0), axis=1
    )
    named = jnp.sum(
        (owner_table.reshape(model_count, per_slab) == model_index).astype(jnp.int32), axis=1
    )
    rank = jnp.sum(
        jnp.where(owner_ids[None, :] < owner_ids[:, None], named[None, :], 0), axis=1
    )
    slot_ids = jnp.arange(CAP, dtype=jnp.int32)
    match = (rank[None, :] == slot_ids[:, None]) & (named[None, :] > 0)
    slot_index = jnp.sum(jnp.where(match, owner_ids[None, :], 0), axis=1)
    return send_index, slot_index, jnp.sum(named).reshape(1)


def exchange(value, bits, data_count):
    return lax.ppermute(value, "dp", [(d, d ^ bits) for d in range(data_count)])


def exchange_all(values, data_count):
    return [values[0]] + [
        exchange(values[bits], bits, data_count) for bits in range(1, data_count)
    ]


def on_device(gradients, owner_table):
    data_count = lax.axis_size("dp")
    model_count = lax.axis_size("mp")
    data_index = lax.axis_index("dp")
    model_index = lax.axis_index("mp")
    row_blocks = gradients.shape[1] // BLOCK
    blocks = gradients[0].reshape(row_blocks, BLOCK, BLOCK)
    device = data_index.astype(jnp.int32).reshape(1)
    send_index, slot_index, load = make_plan(
        owner_table, model_index, model_count, 2 * row_blocks
    )

    groups = []
    for group in range(2):
        own, away = gram_blocks(blocks, device, group * row_blocks // 2, row_blocks // 2)
        got = exchange(away, 1, data_count)
        parts = []
        for part in range(2):
            first = own[part, :2].astype(F32) + got[part, :2].astype(F32)
            step = exchange(first.astype(BF16), FIRST_BITS[part], data_count)
            second = own[part, 3:].astype(F32) + got[part, 3:].astype(F32) + step[1:].astype(F32)
            parts.append((step, exchange(second.astype(BF16), SECOND_BITS[part], data_count)))
        groups.append((own, got, parts))

    outgoing, *home = sum_and_send(device, send_index, groups)
    incoming = lax.all_to_all(outgoing, "mp", split_axis=0, concat_axis=0, tiled=True)

    rows = home_roots(device, exchange_all(home, data_count), data_count)
    slab_roots = finish_rows(device, exchange_all(rows, data_count))

    slots = slot_pick(device, slot_index, incoming)
    root_stacks = owner_roots(device, load, exchange_all(slots, data_count), data_count)
    return (root_stacks[None], slab_roots)


def solution(mesh):
    placed = (P("dp", None, "mp"), P())
    return jax.shard_map(
        on_device,
        mesh=mesh,
        in_specs=placed,
        out_specs=(P("mp", "dp", None, None), P(None, "dp", "mp")),
        check_vma=False,
    )
```

```python
import functools

import jax
import jax.numpy as jnp
from jax import lax
from jax.experimental import pallas as pl
from jax.experimental.pallas import tpu as pltpu
from jax.sharding import PartitionSpec as P


CAP = 24
BLOCK = 512
TILE = 128
DEVICES = 8
UPPER = [(0, 0), (0, 1), (0, 2), (0, 3), (1, 1), (1, 2), (1, 3), (2, 2), (2, 3), (3, 3)]
PACKED_ROWS = len(UPPER) * TILE
CHUNK = PACKED_ROWS // DEVICES
PIECE = CHUNK // 2
ROWS = BLOCK // DEVICES
ORDERS = ((1, 2, 0, 3), (3, 2, 0, 1))
FIRST_BITS = (2, 6)
SECOND_BITS = (6, 2)
VMEM_LIMIT = 24 * 2**20
GRAM_VMEM_LIMIT = 24 * 2**20
INTERPRET = False
F32 = jnp.float32
BF16 = jnp.bfloat16


def rows_of(block):
    return slice(block * TILE, (block + 1) * TILE)


def dot(first, second, dims=((1,), (0,))):
    return lax.dot_general(first, second, (dims, ((), ())), preferred_element_type=F32)


def iota(shape, axis):
    return lax.broadcasted_iota(jnp.int32, shape, axis)


def whole(memory_space=pltpu.VMEM):
    return pl.BlockSpec(memory_space=memory_space)


def params(limit=None):
    return pltpu.CompilerParams(vmem_limit_bytes=limit or VMEM_LIMIT)


def position(code_ref, model_count):
    return code_ref[0] // model_count, code_ref[0] % model_count


def cost(flops, moved):
    return pl.CostEstimate(flops=int(flops), bytes_accessed=int(moved), transcendentals=0)


def gram_kernel(model_count, code_ref, block_ref, own_ref, away_ref, stack_ref):
    block = block_ref[0]
    half = BLOCK // 2
    device, _ = position(code_ref, model_count)
    core = device & 1
    along = device >> 1
    for side in range(2):
        dims = ((1,), (1,)) if side == 0 else ((0,), (0,))
        low = block[:half] if side == 0 else block[:, :half]
        high = block[half:] if side == 0 else block[:, half:]
        right = dot(block, high, dims).astype(BF16)
        corner = dot(low, low, dims).astype(BF16)
        for index, (row, column) in enumerate(UPPER):
            if column >= 2:
                piece = right[rows_of(row), rows_of(column - 2)]
            else:
                piece = corner[rows_of(row), rows_of(column)]
            stack_ref[rows_of(index)] = piece
        for chip in range(4):
            offset = chip ^ along
            for part in range(2):
                place = jnp.int32(0)
                for spot, value in enumerate(ORDERS[part]):
                    place = jnp.where(offset == value, spot, place)
                even = stack_ref[pl.ds((4 * chip + part) * PIECE, PIECE)]
                odd = stack_ref[pl.ds((4 * chip + 2 + part) * PIECE, PIECE)]
                own_ref[part, place, side] = jnp.where(core == 0, even, odd)
                away_ref[part, place, side] = jnp.where(core == 0, odd, even)


def gram_blocks(blocks, code, model_count, first, count):
    shape = jax.ShapeDtypeStruct((2, 4, 2 * count, PIECE, TILE), BF16)
    out_spec = pl.BlockSpec((2, 4, 2, PIECE, TILE), lambda step, code_ref: (0, 0, step, 0, 0))
    return pl.pallas_call(
        functools.partial(gram_kernel, model_count),
        out_shape=(shape, shape),
        grid_spec=pltpu.PrefetchScalarGridSpec(
            num_scalar_prefetch=1,
            grid=(count,),
            in_specs=[
                pl.BlockSpec((1, BLOCK, BLOCK), lambda step, code_ref: (first + step, 0, 0))
            ],
            out_specs=[out_spec, out_spec],
            scratch_shapes=[pltpu.VMEM((PACKED_ROWS, TILE), BF16)],
        ),
        interpret=INTERPRET,
        compiler_params=params(GRAM_VMEM_LIMIT),
        cost_estimate=cost(3 * count * BLOCK**3, count * 5 * 2**18),
    )(code, blocks)


def plan_kernel(model_count, code_ref, table_ref, plan_ref):
    _, model = position(code_ref, model_count)
    for slot in range(CAP + 1):
        plan_ref[slot] = 0
    per_slab = table_ref.shape[0] // model_count

    def slab_step(slab, count):
        named = jnp.int32(0)
        for stat in range(per_slab):
            named = named | jnp.where(table_ref[slab * per_slab + stat] == model, 1, 0)

        @pl.when(named > 0)
        def _():
            plan_ref[count] = slab

        return count + named

    plan_ref[CAP] = lax.fori_loop(0, model_count, slab_step, jnp.int32(0))


def make_plan(code, owner_table, model_count):
    return pl.pallas_call(
        functools.partial(plan_kernel, model_count),
        in_specs=[whole(pltpu.SMEM), whole(pltpu.SMEM)],
        out_specs=whole(pltpu.SMEM),
        out_shape=jax.ShapeDtypeStruct((CAP + 1,), jnp.int32),
        interpret=INTERPRET,
        compiler_params=params(2**20),
        name="make_plan",
        cost_estimate=cost(2**22, 2**12),
    )(code, owner_table)


def sum_kernel(model_count, code_ref, table_ref, *refs):
    sources = refs[:8]
    outgoing_ref, *home_refs = refs[8 : 9 + DEVICES]
    mine_ref, send_ref, out_sems, home_sems = refs[9 + DEVICES :]
    device, model = position(code_ref, model_count)
    count = sources[0].shape[0]
    per_slab = 2 * count
    for group in range(2):
        for part in range(2):
            partial_ref, last_ref = sources[4 * group + 2 * part : 4 * group + 2 * part + 2]
            value = partial_ref[...] + last_ref[0].astype(F32)
            mine_ref[group * count : (group + 1) * count, part * PIECE : (part + 1) * PIECE] = (
                value.astype(BF16)
            )
    for owner in range(model_count):
        send_ref[owner] = 0
    for stat in range(per_slab):
        send_ref[table_ref[model * per_slab + stat]] = stat
    copies = []
    for owner in range(model_count):
        copies.append(
            pltpu.make_async_copy(
                mine_ref.at[send_ref[owner]], outgoing_ref.at[owner], out_sems.at[owner]
            )
        )
    for bits, home_ref in enumerate(home_refs):
        home = device ^ bits
        copies.append(
            pltpu.make_async_copy(mine_ref.at[pl.ds(2 * home, 2)], home_ref, home_sems.at[bits])
        )
    for copy in copies:
        copy.start()
    for copy in copies:
        copy.wait()


def sum_and_send(code, owner_table, sources, model_count):
    count = sources[0].shape[0]
    home = jax.ShapeDtypeStruct((2, CHUNK, TILE), BF16)
    return pl.pallas_call(
        functools.partial(sum_kernel, model_count),
        in_specs=[whole(pltpu.SMEM), whole(pltpu.SMEM)] + [whole()] * 8,
        out_specs=[whole(pltpu.HBM)] * (1 + DEVICES),
        out_shape=[jax.ShapeDtypeStruct((model_count, CHUNK, TILE), BF16)] + [home] * DEVICES,
        scratch_shapes=[
            pltpu.VMEM((2 * count, CHUNK, TILE), BF16),
            pltpu.SMEM((model_count,), jnp.int32),
            pltpu.SemaphoreType.DMA((model_count,)),
            pltpu.SemaphoreType.DMA((DEVICES,)),
        ],
        interpret=INTERPRET,
        compiler_params=params(),
        name="sum_and_send",
        cost_estimate=cost(2**21, 2**22),
    )(code, owner_table, *sources)


def slot_kernel(plan_ref, source_ref, out_ref, sems):
    copies = []
    for slot in range(CAP):
        copies.append(
            pltpu.make_async_copy(source_ref.at[plan_ref[slot]], out_ref.at[slot], sems.at[slot])
        )
    for copy in copies:
        copy.start()
    for copy in copies:
        copy.wait()


def slot_pick(plan, incoming):
    return pl.pallas_call(
        slot_kernel,
        in_specs=[whole(pltpu.SMEM), whole()],
        out_specs=whole(pltpu.HBM),
        out_shape=jax.ShapeDtypeStruct((CAP, CHUNK, TILE), BF16),
        scratch_shapes=[pltpu.SemaphoreType.DMA((CAP,))],
        interpret=INTERPRET,
        compiler_params=params(8 * 2**20),
        name="slot_pick",
        cost_estimate=cost(2**21, 2**22),
    )(plan, incoming)


def total(value):
    return jnp.sum(jnp.sum(value, axis=0, keepdims=True), axis=1, keepdims=True)


def root_of(chunk_piece, data_count, stat_ref, pair_ref):
    for index, (row, column) in enumerate(UPPER):
        start, stop = index * TILE, (index + 1) * TILE
        while start < stop:
            chunk = start // CHUNK
            end = min(stop, (chunk + 1) * CHUNK)
            piece = chunk_piece(chunk, start - chunk * CHUNK, end - chunk * CHUNK)
            base = row * TILE + start - index * TILE
            stat_ref[base : base + end - start, rows_of(column)] = piece
            start = end
        if row != column:
            stat_ref[rows_of(column), rows_of(row)] = stat_ref[rows_of(row), rows_of(column)].T
    on_diagonal = iota((BLOCK, BLOCK), 0) == iota((BLOCK, BLOCK), 1)
    statistic = stat_ref[...] * (1.0 / data_count)
    diagonal_mean = total(jnp.where(on_diagonal, statistic, 0.0)) * (1.0 / BLOCK)
    damped = statistic + jnp.where(on_diagonal, 0.1 * diagonal_mean, 0.0)
    mean_square = total(damped * damped) * (1.0 / BLOCK**2)
    norm_scale = BLOCK * jnp.sqrt(mean_square + 1e-06)
    root_scale = lax.rsqrt(jnp.sqrt(norm_scale))
    first = damped * (1.0 / norm_scale)
    first_small = first.astype(BF16)
    part = (dot(first_small, first_small) * 0.0625 - 0.625 * first).astype(BF16)
    twice = 1.5625 * first + dot(part, first_small)
    twice_small = twice.astype(BF16)
    pair_ref[:BLOCK] = part
    pair_ref[BLOCK:] = twice_small
    both = dot(pair_ref[...], twice_small)
    second = 1.5625 * twice + both[:BLOCK]
    pair = (both[BLOCK:] * 0.0625 - 0.3125 * (first + second)).astype(BF16)
    second_small = second.astype(BF16)
    part = (dot(second_small, second_small) * 0.0625 - 0.625 * second).astype(BF16)
    twice = 1.5625 * second + dot(part, second_small)
    third = 1.5625 * twice + dot(part, twice.astype(BF16))
    rest = 1.25 * pair.astype(F32) - 0.390625 * third - 0.25 * dot(pair, third.astype(BF16))
    return rest * root_scale, 1.953125 * root_scale, on_diagonal


def home_kernel(data_count, model_count, code_ref, *refs):
    sources, row_refs = refs[:DEVICES], refs[DEVICES : 2 * DEVICES]
    rows_ref, stack_ref, stat_ref, pair_ref = refs[2 * DEVICES :]
    device, _ = position(code_ref, model_count)
    row_ids = iota((BLOCK, BLOCK), 0)
    spare = (row_ids % ROWS == 1) & (iota((BLOCK, BLOCK), 1) == row_ids - 1)
    for stat in range(2):
        for bits, ref in enumerate(sources):
            stack_ref[device ^ bits] = ref[stat].astype(F32)
        rest, identity_part, on_diagonal = root_of(
            lambda chunk, start, stop: stack_ref[chunk, start:stop], data_count, stat_ref, pair_ref
        )
        rest_mean = total(jnp.where(on_diagonal, rest, 0.0)) * (1.0 / BLOCK)
        center = (identity_part + rest_mean).astype(BF16).astype(F32)
        rest = rest + jnp.where(on_diagonal, identity_part - center, 0.0)
        sent = jnp.where(spare, center, rest).astype(BF16)
        for home in range(DEVICES):
            rows_ref[home] = sent[home * ROWS : (home + 1) * ROWS]
        for bits, row_ref in enumerate(row_refs):
            row_ref[stat] = rows_ref[device ^ bits]


def home_roots(code, sources, data_count, model_count):
    return pl.pallas_call(
        functools.partial(home_kernel, data_count, model_count),
        in_specs=[whole(pltpu.SMEM)] + [whole()] * DEVICES,
        out_specs=[whole()] * DEVICES,
        out_shape=[jax.ShapeDtypeStruct((2, ROWS, BLOCK), BF16)] * DEVICES,
        scratch_shapes=[
            pltpu.VMEM((DEVICES, ROWS, BLOCK), BF16),
            pltpu.VMEM((DEVICES, CHUNK, TILE), F32),
            pltpu.VMEM((BLOCK, BLOCK), F32),
            pltpu.VMEM((2 * BLOCK, BLOCK), BF16),
        ],
        interpret=INTERPRET,
        compiler_params=params(),
        name="home_roots",
        cost_estimate=cost(2 * 8 * 2 * BLOCK**3, 2**22),
    )(code, *sources)


def owner_kernel(data_count, model_count, code_ref, plan_ref, source_ref, out_ref, stat_ref, pair_ref):
    device, _ = position(code_ref, model_count)
    slot = pl.program_id(0)
    keep = pl.num_programs(0) * device + slot < plan_ref[CAP]

    @pl.when(keep)
    def _():
        rest, identity_part, on_diagonal = root_of(
            lambda chunk, start, stop: source_ref[chunk, 0, start:stop].astype(F32),
            data_count,
            stat_ref,
            pair_ref,
        )
        out_ref[0] = rest + jnp.where(on_diagonal, identity_part, 0.0)

    @pl.when(jnp.logical_not(keep))
    def _():
        out_ref[...] = jnp.zeros_like(out_ref)


def owner_roots(code, plan, source, data_count, model_count):
    slots = source.shape[1]
    return pl.pallas_call(
        functools.partial(owner_kernel, data_count, model_count),
        grid=(slots,),
        in_specs=[
            whole(pltpu.SMEM),
            whole(pltpu.SMEM),
            pl.BlockSpec((DEVICES, 1, CHUNK, TILE), lambda slot: (0, slot, 0, 0)),
        ],
        out_specs=pl.BlockSpec((1, BLOCK, BLOCK), lambda slot: (slot, 0, 0)),
        out_shape=jax.ShapeDtypeStruct((slots, BLOCK, BLOCK), F32),
        scratch_shapes=[
            pltpu.VMEM((BLOCK, BLOCK), F32),
            pltpu.VMEM((2 * BLOCK, BLOCK), BF16),
        ],
        interpret=INTERPRET,
        compiler_params=params(),
        name="owner_roots",
        cost_estimate=cost(3 * 8 * 2 * BLOCK**3, 2**22),
    )(code, plan, source)


def finish_kernel(model_count, code_ref, *refs):
    out_ref = refs[-1]
    device, _ = position(code_ref, model_count)
    first = device * ROWS
    row_ids = iota((ROWS, BLOCK), 0)
    column_ids = iota((ROWS, BLOCK), 1) - first
    spare = (row_ids == 1) & (column_ids == 0)
    mirror = (row_ids == 0) & (column_ids == 1)
    on_diagonal = row_ids == column_ids
    for bits, ref in enumerate(refs[:-1]):
        home = device ^ bits
        for stat in range(2):
            value = ref[stat].astype(F32)
            center = total(jnp.where(spare[:8], value[:8], 0.0))
            mirrored = total(jnp.where(mirror[:8], value[:8], 0.0))
            value = jnp.where(spare, mirrored, value)
            out_ref[2 * home + stat] = value + jnp.where(on_diagonal, center, 0.0)


def finish_rows(code, rows, model_count):
    return pl.pallas_call(
        functools.partial(finish_kernel, model_count),
        in_specs=[whole(pltpu.SMEM)] + [whole()] * DEVICES,
        out_specs=whole(),
        out_shape=jax.ShapeDtypeStruct((2 * DEVICES, ROWS, BLOCK), F32),
        interpret=INTERPRET,
        compiler_params=params(),
        name="finish_rows",
        cost_estimate=cost(2**21, 2**22),
    )(code, *rows)


def exchange(value, bits, data_count):
    return lax.ppermute(value, "dp", [(d, d ^ bits) for d in range(data_count)])


def exchange_all(values, data_count):
    return [values[0]] + [
        exchange(values[bits], bits, data_count) for bits in range(1, data_count)
    ]


def program(gradients, owner_table):
    data_count = lax.axis_size("dp")
    model_count = lax.axis_size("mp")
    row_blocks = gradients.shape[1] // BLOCK
    blocks = gradients[0].reshape(row_blocks, BLOCK, BLOCK)
    code = (lax.axis_index("dp") * model_count + lax.axis_index("mp")).reshape(1)

    sources = []
    for group in range(2):
        own, away = gram_blocks(blocks, code, model_count, group * row_blocks // 2, row_blocks // 2)
        got = exchange(away, 1, data_count)
        for part in range(2):
            first = own[part, :2].astype(F32) + got[part, :2].astype(F32)
            step = exchange(first.astype(BF16), FIRST_BITS[part], data_count)
            second = own[part, 3:].astype(F32) + got[part, 3:].astype(F32) + step[1:].astype(F32)
            last = exchange(second.astype(BF16), SECOND_BITS[part], data_count)
            sources.append(
                own[part, 2].astype(F32) + got[part, 2].astype(F32) + step[0].astype(F32)
            )
            sources.append(last)

    plan = make_plan(code, owner_table, model_count)
    outgoing, *home = sum_and_send(code, owner_table, sources, model_count)
    incoming = lax.all_to_all(outgoing, "mp", split_axis=0, concat_axis=0, tiled=True)

    rows = list(home_roots(code, exchange_all(home, data_count), data_count, model_count))
    incoming, rows[0] = lax.optimization_barrier((incoming, rows[0]))
    rows = exchange_all(rows, data_count)
    slab_roots = finish_rows(code, rows, model_count)

    slots = slot_pick(plan, incoming)
    stacked = lax.all_to_all(slots, "dp", split_axis=0, concat_axis=0, tiled=True)
    stacked = stacked.reshape(data_count, CAP // data_count, CHUNK, TILE)
    root_stacks = owner_roots(code, plan, stacked, data_count, model_count)
    return (root_stacks[None], slab_roots)


def solution(mesh):
    placed = (P("dp", None, "mp"), P())
    return jax.shard_map(
        program,
        mesh=mesh,
        in_specs=placed,
        out_specs=(P("mp", "dp", None, None), P(None, "dp", "mp")),
        check_vma=False,
    )
```

```python
import functools

import jax
import jax.numpy as jnp
from jax import lax
from jax.experimental import pallas as pl
from jax.experimental.pallas import tpu as pltpu
from jax.sharding import PartitionSpec as P


CAP = 24
BLOCK = 512
TILE = 128
DEVICES = 8
ABOVE = [(0, 1), (0, 2), (0, 3), (1, 2), (1, 3), (2, 3)]
PACKED_ROWS = 9 * TILE
CHUNK = PACKED_ROWS // DEVICES
CUTS = (80, 64)
ROWS = BLOCK // DEVICES
ORDERS = ((1, 2, 0, 3), (3, 2, 0, 1))
FIRST_BITS = (2, 6)
SECOND_BITS = (6, 2)
VMEM_LIMIT = 24 * 2**20
INTERPRET = False
F32 = jnp.float32
BF16 = jnp.bfloat16


def rows_of(block):
    return slice(block * TILE, (block + 1) * TILE)


def dot(first, second, dims=((1,), (0,))):
    return lax.dot_general(first, second, (dims, ((), ())), preferred_element_type=F32)


def iota(shape, axis):
    return lax.broadcasted_iota(jnp.int32, shape, axis)


def whole(memory_space=pltpu.VMEM):
    return pl.BlockSpec(memory_space=memory_space)


def params(limit=VMEM_LIMIT):
    return pltpu.CompilerParams(vmem_limit_bytes=limit)


def position(code_ref, model_count):
    return code_ref[0] // model_count, code_ref[0] % model_count


def cost(flops, moved):
    return pl.CostEstimate(flops=int(flops), bytes_accessed=int(moved), transcendentals=0)


def gram_step(code_ref, model_count, cut, block, own_ref, away_ref, stack_ref):
    half = BLOCK // 2
    device, _ = position(code_ref, model_count)
    core = device & 1
    along = device >> 1
    row_ids, column_ids = iota((TILE, TILE), 0), iota((TILE, TILE), 1)
    last_row = row_ids == TILE - 1
    for side in range(2):
        dims = ((1,), (1,)) if side == 0 else ((0,), (0,))
        low = block[:half] if side == 0 else block[:, :half]
        high = block[half:] if side == 0 else block[:, half:]
        right = dot(block, high, dims)
        corner = dot(low, low, dims)

        def tile(row, column):
            if column >= 2:
                return right[rows_of(row), rows_of(column - 2)]
            return corner[rows_of(row), rows_of(column)]

        tiles = [tile(row, column) for row, column in ABOVE]
        inner = tile(1, 1)
        diagonal = jnp.sum(jnp.where(row_ids == column_ids, inner, 0.0), axis=0, keepdims=True)
        corner_end = inner[TILE - 1 :, TILE - 1 :]
        tiles.append(jnp.where(column_ids >= row_ids, tile(0, 0), inner))
        tiles.append(jnp.where(last_row & (column_ids < TILE - 1), diagonal, tile(2, 2)))
        tiles.append(jnp.where(last_row & (column_ids == 0), corner_end, tile(3, 3)))
        for index, value in enumerate(tiles):
            stack_ref[rows_of(index)] = value.astype(BF16)
        for chip in range(4):
            offset = chip ^ along
            for part, (start, stop) in enumerate(((0, cut), (cut, CHUNK))):
                place = jnp.int32(0)
                for spot, value in enumerate(ORDERS[part]):
                    place = jnp.where(offset == value, spot, place)
                base = 2 * chip * CHUNK
                even = stack_ref[base + start : base + stop]
                odd = stack_ref[base + CHUNK + start : base + CHUNK + stop]
                own_ref[place, side, start:stop] = jnp.where(core == 0, even, odd)
                away_ref[place, side, start:stop] = jnp.where(core == 0, odd, even)


def gram_kernel(model_count, cut, code_ref, block_ref, own_ref, away_ref, stack_ref):
    gram_step(code_ref, model_count, cut, block_ref[0], own_ref, away_ref, stack_ref)


def gram_blocks(blocks, code, model_count, first, count, cut):
    shape = jax.ShapeDtypeStruct((4, 2 * count, CHUNK, TILE), BF16)
    out_spec = pl.BlockSpec((4, 2, CHUNK, TILE), lambda step, code_ref: (0, step, 0, 0))
    in_spec = pl.BlockSpec((1, BLOCK, BLOCK), lambda step, code_ref: (first + step, 0, 0))
    return pl.pallas_call(
        functools.partial(gram_kernel, model_count, cut),
        out_shape=(shape, shape),
        grid_spec=pltpu.PrefetchScalarGridSpec(
            num_scalar_prefetch=1,
            grid=(count,),
            in_specs=[in_spec],
            out_specs=[out_spec, out_spec],
            scratch_shapes=[pltpu.VMEM((PACKED_ROWS, TILE), BF16)],
        ),
        interpret=INTERPRET,
        compiler_params=params(),
        cost_estimate=cost(3 * count * BLOCK**3, count * 5 * 2**18),
    )(code, blocks)


def plan_kernel(model_count, code_ref, table_ref, plan_ref):
    _, model = position(code_ref, model_count)
    for slot in range(CAP + 1):
        plan_ref[slot] = 0
    per_slab = table_ref.shape[0] // model_count

    def slab_step(slab, count):
        named = jnp.int32(0)
        for stat in range(per_slab):
            named = named | jnp.where(table_ref[slab * per_slab + stat] == model, 1, 0)

        @pl.when(named > 0)
        def _():
            plan_ref[count] = slab

        return count + named

    plan_ref[CAP] = lax.fori_loop(0, model_count, slab_step, jnp.int32(0))


def make_plan(code, owner_table, model_count):
    return pl.pallas_call(
        functools.partial(plan_kernel, model_count),
        in_specs=[whole(pltpu.SMEM), whole(pltpu.SMEM)],
        out_specs=whole(pltpu.SMEM),
        out_shape=jax.ShapeDtypeStruct((CAP + 1,), jnp.int32),
        interpret=INTERPRET,
        compiler_params=params(2**20),
        name="make_plan",
        cost_estimate=cost(2**22, 2**12),
    )(code, owner_table)


def sum_kernel(model_count, code_ref, table_ref, *refs):
    sources = refs[:8]
    outgoing_ref, *home_refs = refs[8 : 9 + DEVICES]
    mine_ref, send_ref, out_sems, home_sems = refs[9 + DEVICES :]
    device, model = position(code_ref, model_count)
    count = sources[0].shape[0]
    per_slab = 2 * count
    for group, cut in enumerate(CUTS):
        for part, (start, stop) in enumerate(((0, cut), (cut, CHUNK))):
            partial_ref, last_ref = sources[4 * group + 2 * part : 4 * group + 2 * part + 2]
            value = partial_ref[...] + last_ref[0].astype(F32)
            mine_ref[group * count : (group + 1) * count, start:stop] = value.astype(BF16)
    for owner in range(model_count):
        send_ref[owner] = 0
    for stat in range(per_slab):
        send_ref[table_ref[model * per_slab + stat]] = stat
    copies = []
    for owner in range(model_count):
        copies.append(
            pltpu.make_async_copy(
                mine_ref.at[send_ref[owner]], outgoing_ref.at[owner], out_sems.at[owner]
            )
        )
    for bits, home_ref in enumerate(home_refs):
        home = device ^ bits
        copies.append(
            pltpu.make_async_copy(mine_ref.at[pl.ds(2 * home, 2)], home_ref, home_sems.at[bits])
        )
    for copy in copies:
        copy.start()
    for copy in copies:
        copy.wait()


def sum_and_send(code, owner_table, sources, model_count):
    count = sources[0].shape[0]
    home = jax.ShapeDtypeStruct((2, CHUNK, TILE), BF16)
    return pl.pallas_call(
        functools.partial(sum_kernel, model_count),
        in_specs=[whole(pltpu.SMEM), whole(pltpu.SMEM)] + [whole()] * 8,
        out_specs=[whole(pltpu.HBM)] * (1 + DEVICES),
        out_shape=[jax.ShapeDtypeStruct((model_count, CHUNK, TILE), BF16)] + [home] * DEVICES,
        scratch_shapes=[
            pltpu.VMEM((2 * count, CHUNK, TILE), BF16),
            pltpu.SMEM((model_count,), jnp.int32),
            pltpu.SemaphoreType.DMA((model_count,)),
            pltpu.SemaphoreType.DMA((DEVICES,)),
        ],
        interpret=INTERPRET,
        compiler_params=params(),
        name="sum_and_send",
        cost_estimate=cost(2**21, 2**22),
    )(code, owner_table, *sources)


def slot_kernel(plan_ref, source_ref, out_ref, sems):
    copies = []
    for slot in range(CAP):
        copies.append(
            pltpu.make_async_copy(source_ref.at[plan_ref[slot]], out_ref.at[slot], sems.at[slot])
        )
    for copy in copies:
        copy.start()
    for copy in copies:
        copy.wait()


def slot_pick(plan, incoming):
    return pl.pallas_call(
        slot_kernel,
        in_specs=[whole(pltpu.SMEM), whole()],
        out_specs=whole(pltpu.HBM),
        out_shape=jax.ShapeDtypeStruct((CAP, CHUNK, TILE), BF16),
        scratch_shapes=[pltpu.SemaphoreType.DMA((CAP,))],
        interpret=INTERPRET,
        compiler_params=params(8 * 2**20),
        name="slot_pick",
        cost_estimate=cost(2**21, 2**22),
    )(plan, incoming)


def total(value):
    return jnp.sum(jnp.sum(value, axis=0, keepdims=True), axis=1, keepdims=True)


def unpack(stack_ref, stat_ref):
    row_ids, column_ids = iota((TILE, TILE), 0), iota((TILE, TILE), 1)
    last_row = row_ids == TILE - 1
    for index, (row, column) in enumerate(ABOVE):
        value = stack_ref[rows_of(index)]
        stat_ref[rows_of(row), rows_of(column)] = value
        stat_ref[rows_of(column), rows_of(row)] = value.T
    shared, third, fourth = [stack_ref[rows_of(index)] for index in (6, 7, 8)]
    mirrored = shared.T
    diagonal = jnp.where(column_ids == TILE - 1, fourth[TILE - 1 :, :1], third[TILE - 1 :])
    stat_ref[rows_of(0), rows_of(0)] = jnp.where(column_ids >= row_ids, shared, mirrored)
    stat_ref[rows_of(1), rows_of(1)] = jnp.where(
        row_ids == column_ids, diagonal, jnp.where(column_ids < row_ids, shared, mirrored)
    )
    stat_ref[rows_of(2), rows_of(2)] = jnp.where(last_row, third.T, third)
    stat_ref[rows_of(3), rows_of(3)] = jnp.where(last_row, fourth.T, fourth)


def root_of(data_count, stack_ref, stat_ref, pair_ref):
    unpack(stack_ref, stat_ref)
    on_diagonal = iota((BLOCK, BLOCK), 0) == iota((BLOCK, BLOCK), 1)
    statistic = stat_ref[...] * (1.0 / data_count)
    diagonal_mean = total(jnp.where(on_diagonal, statistic, 0.0)) * (1.0 / BLOCK)
    damped = statistic + jnp.where(on_diagonal, 0.1 * diagonal_mean, 0.0)
    mean_square = total(damped * damped) * (1.0 / BLOCK**2)
    norm_scale = BLOCK * jnp.sqrt(mean_square + 1e-06)
    root_scale = lax.rsqrt(jnp.sqrt(norm_scale))
    first = damped * (1.0 / norm_scale)
    first_small = first.astype(BF16)
    part = (dot(first_small, first_small) * 0.0625 - 0.625 * first).astype(BF16)
    twice = 1.5625 * first + dot(part, first_small)
    twice_small = twice.astype(BF16)
    pair_ref[:BLOCK] = part
    pair_ref[BLOCK:] = twice_small
    both = dot(pair_ref[...], twice_small)
    second = 1.5625 * twice + both[:BLOCK]
    pair = (both[BLOCK:] * 0.0625 - 0.3125 * (first + second)).astype(BF16)
    second_small = second.astype(BF16)
    part = (dot(second_small, second_small) * 0.0625 - 0.625 * second).astype(BF16)
    twice = 1.5625 * second + dot(part, second_small)
    third = 1.5625 * twice + dot(part, twice.astype(BF16))
    rest = 1.25 * pair.astype(F32) - 0.390625 * third - 0.25 * dot(pair, third.astype(BF16))
    return rest * root_scale, 1.953125 * root_scale, on_diagonal


def home_kernel(data_count, model_count, code_ref, *refs):
    sources, row_refs = refs[:DEVICES], refs[DEVICES : 2 * DEVICES]
    rows_ref, stack_ref, stat_ref, pair_ref = refs[2 * DEVICES :]
    device, _ = position(code_ref, model_count)
    row_ids = iota((BLOCK, BLOCK), 0)
    spare = (row_ids % ROWS == 1) & (iota((BLOCK, BLOCK), 1) == row_ids - 1)
    for stat in range(2):
        for bits, ref in enumerate(sources):
            start = pl.multiple_of((device ^ bits) * CHUNK, 16)
            stack_ref[pl.ds(start, CHUNK)] = ref[stat].astype(F32)
        rest, identity_part, on_diagonal = root_of(data_count, stack_ref, stat_ref, pair_ref)
        rest_mean = total(jnp.where(on_diagonal, rest, 0.0)) * (1.0 / BLOCK)
        center = (identity_part + rest_mean).astype(BF16).astype(F32)
        rest = rest + jnp.where(on_diagonal, identity_part - center, 0.0)
        sent = jnp.where(spare, center, rest).astype(BF16)
        for home in range(DEVICES):
            rows_ref[home] = sent[home * ROWS : (home + 1) * ROWS]
        for bits, row_ref in enumerate(row_refs):
            row_ref[stat] = rows_ref[device ^ bits]


def home_roots(code, sources, data_count, model_count):
    return pl.pallas_call(
        functools.partial(home_kernel, data_count, model_count),
        in_specs=[whole(pltpu.SMEM)] + [whole()] * DEVICES,
        out_specs=[whole()] * DEVICES,
        out_shape=[jax.ShapeDtypeStruct((2, ROWS, BLOCK), BF16)] * DEVICES,
        scratch_shapes=[
            pltpu.VMEM((DEVICES, ROWS, BLOCK), BF16),
            pltpu.VMEM((PACKED_ROWS, TILE), F32),
            pltpu.VMEM((BLOCK, BLOCK), F32),
            pltpu.VMEM((2 * BLOCK, BLOCK), BF16),
        ],
        interpret=INTERPRET,
        compiler_params=params(),
        name="home_roots",
        cost_estimate=cost(2 * 8 * 2 * BLOCK**3, 2**22),
    )(code, *sources)


def owner_kernel(
    data_count, model_count, code_ref, plan_ref, source_ref, out_ref, stack_ref, stat_ref, pair_ref
):
    device, _ = position(code_ref, model_count)
    slot = pl.program_id(0)
    keep = pl.num_programs(0) * device + slot < plan_ref[CAP]

    @pl.when(keep)
    def _():
        for chunk in range(DEVICES):
            stack_ref[chunk * CHUNK : (chunk + 1) * CHUNK] = source_ref[chunk, 0].astype(F32)
        rest, identity_part, on_diagonal = root_of(data_count, stack_ref, stat_ref, pair_ref)
        out_ref[0] = rest + jnp.where(on_diagonal, identity_part, 0.0)

    @pl.when(jnp.logical_not(keep))
    def _():
        out_ref[...] = jnp.zeros_like(out_ref)


def owner_roots(code, plan, source, data_count, model_count):
    slots = source.shape[1]
    return pl.pallas_call(
        functools.partial(owner_kernel, data_count, model_count),
        grid=(slots,),
        in_specs=[
            whole(pltpu.SMEM),
            whole(pltpu.SMEM),
            pl.BlockSpec((DEVICES, 1, CHUNK, TILE), lambda slot: (0, slot, 0, 0)),
        ],
        out_specs=pl.BlockSpec((1, BLOCK, BLOCK), lambda slot: (slot, 0, 0)),
        out_shape=jax.ShapeDtypeStruct((slots, BLOCK, BLOCK), F32),
        scratch_shapes=[
            pltpu.VMEM((PACKED_ROWS, TILE), F32),
            pltpu.VMEM((BLOCK, BLOCK), F32),
            pltpu.VMEM((2 * BLOCK, BLOCK), BF16),
        ],
        interpret=INTERPRET,
        compiler_params=params(),
        name="owner_roots",
        cost_estimate=cost(3 * 8 * 2 * BLOCK**3, 2**22),
    )(code, plan, source)


def finish_kernel(model_count, code_ref, *refs):
    out_ref = refs[-1]
    device, _ = position(code_ref, model_count)
    first = device * ROWS
    row_ids = iota((ROWS, BLOCK), 0)
    column_ids = iota((ROWS, BLOCK), 1) - first
    spare = (row_ids == 1) & (column_ids == 0)
    mirror = (row_ids == 0) & (column_ids == 1)
    on_diagonal = row_ids == column_ids
    for bits, ref in enumerate(refs[:-1]):
        home = device ^ bits
        for stat in range(2):
            value = ref[stat].astype(F32)
            center = total(jnp.where(spare[:8], value[:8], 0.0))
            mirrored = total(jnp.where(mirror[:8], value[:8], 0.0))
            value = jnp.where(spare, mirrored, value)
            out_ref[2 * home + stat] = value + jnp.where(on_diagonal, center, 0.0)


def finish_rows(code, rows, model_count):
    return pl.pallas_call(
        functools.partial(finish_kernel, model_count),
        in_specs=[whole(pltpu.SMEM)] + [whole()] * DEVICES,
        out_specs=whole(),
        out_shape=jax.ShapeDtypeStruct((2 * DEVICES, ROWS, BLOCK), F32),
        interpret=INTERPRET,
        compiler_params=params(),
        name="finish_rows",
        cost_estimate=cost(2**21, 2**22),
    )(code, *rows)


def exchange(value, bits, data_count):
    return lax.ppermute(value, "dp", [(d, d ^ bits) for d in range(data_count)])


def exchange_all(values, data_count):
    return [values[0]] + [
        exchange(values[bits], bits, data_count) for bits in range(1, data_count)
    ]


def program(gradients, owner_table):
    data_count = lax.axis_size("dp")
    model_count = lax.axis_size("mp")
    row_blocks = gradients.shape[1] // BLOCK
    blocks = gradients[0].reshape(row_blocks, BLOCK, BLOCK)
    code = (lax.axis_index("dp") * model_count + lax.axis_index("mp")).reshape(1)

    sources = []
    half = row_blocks // 2
    gram_code = code
    for group, cut in enumerate(CUTS):
        own, away = gram_blocks(blocks, gram_code, model_count, group * half, half, cut)
        if group == 0:
            gram_code, away = lax.optimization_barrier((gram_code, away))
        got = exchange(away, 1, data_count)
        for part, rows in enumerate((slice(0, cut), slice(cut, CHUNK))):
            first = own[:2, :, rows].astype(F32) + got[:2, :, rows].astype(F32)
            step = exchange(first.astype(BF16), FIRST_BITS[part], data_count)
            second = own[3:, :, rows].astype(F32) + got[3:, :, rows].astype(F32)
            second = second + step[1:].astype(F32)
            last = exchange(second.astype(BF16), SECOND_BITS[part], data_count)
            third = own[2, :, rows].astype(F32) + got[2, :, rows].astype(F32)
            sources += [third + step[0].astype(F32), last]

    plan = make_plan(code, owner_table, model_count)
    outgoing, *home = sum_and_send(code, owner_table, sources, model_count)
    incoming = lax.all_to_all(outgoing, "mp", split_axis=0, concat_axis=0, tiled=True)

    rows = list(home_roots(code, exchange_all(home, data_count), data_count, model_count))
    incoming, rows[0] = lax.optimization_barrier((incoming, rows[0]))
    rows = exchange_all(rows, data_count)
    slab_roots = finish_rows(code, rows, model_count)

    slots = slot_pick(plan, incoming)
    stacked = lax.all_to_all(slots, "dp", split_axis=0, concat_axis=0, tiled=True)
    stacked = stacked.reshape(data_count, CAP // data_count, CHUNK, TILE)
    root_stacks = owner_roots(code, plan, stacked, data_count, model_count)
    return (root_stacks[None], slab_roots)


def solution(mesh):
    placed = (P("dp", None, "mp"), P())
    return jax.shard_map(
        program,
        mesh=mesh,
        in_specs=placed,
        out_specs=(P("mp", "dp", None, None), P(None, "dp", "mp")),
        check_vma=False,
    )
```

```python
import functools

import jax
import jax.numpy as jnp
from jax import lax
from jax.experimental import pallas as pl
from jax.experimental.pallas import tpu as pltpu
from jax.sharding import PartitionSpec as P


CAP = 24
BLOCK = 512
TILE = 128
DEVICES = 8
ABOVE = [(0, 1), (0, 2), (0, 3), (1, 2), (1, 3), (2, 3)]
PACKED_ROWS = 9 * TILE
CHUNK = PACKED_ROWS // DEVICES
CUTS = (80, 64)
PARTNERS = (0, 4, 5, 6, 7, 2, 3, 1)
ROWS = BLOCK // DEVICES
ORDERS = ((1, 2, 0, 3), (3, 2, 0, 1))
FIRST_BITS = (2, 6)
SECOND_BITS = (6, 2)
VMEM_LIMIT = 24 * 2**20
INTERPRET = False
F32 = jnp.float32
BF16 = jnp.bfloat16


def rows_of(block):
    return slice(block * TILE, (block + 1) * TILE)


def dot(first, second, dims=((1,), (0,))):
    return lax.dot_general(first, second, (dims, ((), ())), preferred_element_type=F32)


def iota(shape, axis):
    return lax.broadcasted_iota(jnp.int32, shape, axis)


def whole(memory_space=pltpu.VMEM):
    return pl.BlockSpec(memory_space=memory_space)


def params(limit=VMEM_LIMIT):
    return pltpu.CompilerParams(vmem_limit_bytes=limit)


def position(code_ref, model_count):
    return code_ref[0] // model_count, code_ref[0] % model_count


def cost(flops, moved):
    return pl.CostEstimate(flops=int(flops), bytes_accessed=int(moved), transcendentals=0)


def gram_step(code_ref, model_count, cut, block, own_ref, away_ref, stack_ref):
    half = BLOCK // 2
    device, _ = position(code_ref, model_count)
    core = device & 1
    along = device >> 1
    row_ids, column_ids = iota((TILE, TILE), 0), iota((TILE, TILE), 1)
    last_row = row_ids == TILE - 1
    for side in range(2):
        dims = ((1,), (1,)) if side == 0 else ((0,), (0,))
        low = block[:half] if side == 0 else block[:, :half]
        high = block[half:] if side == 0 else block[:, half:]
        right = dot(block, high, dims)
        corner = dot(low, low, dims)

        def tile(row, column):
            if column >= 2:
                return right[rows_of(row), rows_of(column - 2)]
            return corner[rows_of(row), rows_of(column)]

        tiles = [tile(row, column) for row, column in ABOVE]
        inner = tile(1, 1)
        diagonal = jnp.sum(jnp.where(row_ids == column_ids, inner, 0.0), axis=0, keepdims=True)
        corner_end = inner[TILE - 1 :, TILE - 1 :]
        tiles.append(jnp.where(column_ids >= row_ids, tile(0, 0), inner))
        tiles.append(jnp.where(last_row & (column_ids < TILE - 1), diagonal, tile(2, 2)))
        tiles.append(jnp.where(last_row & (column_ids == 0), corner_end, tile(3, 3)))
        for index, value in enumerate(tiles):
            stack_ref[rows_of(index)] = value.astype(BF16)
        for chip in range(4):
            offset = chip ^ along
            for part, (start, stop) in enumerate(((0, cut), (cut, CHUNK))):
                place = jnp.int32(0)
                for spot, value in enumerate(ORDERS[part]):
                    place = jnp.where(offset == value, spot, place)
                base = 2 * chip * CHUNK
                even = stack_ref[base + start : base + stop]
                odd = stack_ref[base + CHUNK + start : base + CHUNK + stop]
                own_ref[place, side, start:stop] = jnp.where(core == 0, even, odd)
                away_ref[place, side, start:stop] = jnp.where(core == 0, odd, even)


def gram_kernel(model_count, cut, code_ref, block_ref, own_ref, away_ref, stack_ref):
    gram_step(code_ref, model_count, cut, block_ref[0], own_ref, away_ref, stack_ref)


def gram_blocks(blocks, code, model_count, first, count, cut):
    shape = jax.ShapeDtypeStruct((4, 2 * count, CHUNK, TILE), BF16)
    out_spec = pl.BlockSpec((4, 2, CHUNK, TILE), lambda step, code_ref: (0, step, 0, 0))
    in_spec = pl.BlockSpec((1, BLOCK, BLOCK), lambda step, code_ref: (first + step, 0, 0))
    return pl.pallas_call(
        functools.partial(gram_kernel, model_count, cut),
        out_shape=(shape, shape),
        grid_spec=pltpu.PrefetchScalarGridSpec(
            num_scalar_prefetch=1,
            grid=(count,),
            in_specs=[in_spec],
            out_specs=[out_spec, out_spec],
            scratch_shapes=[pltpu.VMEM((PACKED_ROWS, TILE), BF16)],
        ),
        interpret=INTERPRET,
        compiler_params=params(),
        cost_estimate=cost(3 * count * BLOCK**3, count * 5 * 2**18),
    )(code, blocks)


def plan_kernel(model_count, code_ref, table_ref, plan_ref):
    _, model = position(code_ref, model_count)
    for entry in range(plan_ref.shape[0]):
        plan_ref[entry] = 0
    per_slab = table_ref.shape[0] // model_count
    for stat in range(per_slab):
        plan_ref[CAP + 1 + table_ref[model * per_slab + stat]] = stat

    def slab_step(slab, count):
        named = jnp.int32(0)
        for stat in range(per_slab):
            named = named | jnp.where(table_ref[slab * per_slab + stat] == model, 1, 0)

        @pl.when(named > 0)
        def _():
            plan_ref[count] = slab

        return count + named

    plan_ref[CAP] = lax.fori_loop(0, model_count, slab_step, jnp.int32(0))


def make_plan(code, owner_table, model_count):
    return pl.pallas_call(
        functools.partial(plan_kernel, model_count),
        in_specs=[whole(pltpu.SMEM), whole(pltpu.SMEM)],
        out_specs=whole(pltpu.SMEM),
        out_shape=jax.ShapeDtypeStruct((CAP + 1 + model_count,), jnp.int32),
        interpret=INTERPRET,
        compiler_params=params(2**20),
        name="make_plan",
        cost_estimate=cost(2**22, 2**12),
    )(code, owner_table)


def sum_kernel(model_count, code_ref, plan_ref, *refs):
    sources = refs[:8]
    outgoing_ref, *home_refs = refs[8 : 9 + DEVICES]
    mine_ref, out_sems, home_sems = refs[9 + DEVICES :]
    device, _ = position(code_ref, model_count)
    base = 0
    for group, cut in enumerate(CUTS):
        for part, (start, stop) in enumerate(((0, cut), (cut, CHUNK))):
            partial_ref, last_ref = sources[4 * group + 2 * part : 4 * group + 2 * part + 2]
            value = partial_ref[...] + last_ref[0].astype(F32)
            mine_ref[base : base + value.shape[0], start:stop] = value.astype(BF16)
        base += value.shape[0]
    copies = []
    for owner in range(model_count):
        copies.append(
            pltpu.make_async_copy(
                mine_ref.at[plan_ref[CAP + 1 + owner]], outgoing_ref.at[owner], out_sems.at[owner]
            )
        )
    for bits, home_ref in zip(PARTNERS, home_refs):
        home = device ^ bits
        copies.append(
            pltpu.make_async_copy(mine_ref.at[pl.ds(2 * home, 2)], home_ref, home_sems.at[bits])
        )
    for copy in copies:
        copy.start()
    for copy in copies:
        copy.wait()


def sum_and_send(code, plan, sources, model_count):
    home = jax.ShapeDtypeStruct((2, CHUNK, TILE), BF16)
    return pl.pallas_call(
        functools.partial(sum_kernel, model_count),
        in_specs=[whole(pltpu.SMEM), whole(pltpu.SMEM)] + [whole()] * 8,
        out_specs=[whole(pltpu.HBM)] * (1 + DEVICES),
        out_shape=[jax.ShapeDtypeStruct((model_count, CHUNK, TILE), BF16)] + [home] * DEVICES,
        scratch_shapes=[
            pltpu.VMEM((2 * DEVICES, CHUNK, TILE), BF16),
            pltpu.SemaphoreType.DMA((model_count,)),
            pltpu.SemaphoreType.DMA((DEVICES,)),
        ],
        interpret=INTERPRET,
        compiler_params=params(),
        name="sum_and_send",
        cost_estimate=cost(2**21, 2**22),
    )(code, plan, *sources)


def slot_kernel(model_count, code_ref, plan_ref, source_ref, *slot_refs):
    device, _ = position(code_ref, model_count)
    slots = slot_refs[0].shape[0]
    for bits, slot_ref in zip(PARTNERS, slot_refs):
        home = device ^ bits
        for slot in range(slots):
            slot_ref[slot] = source_ref[plan_ref[slots * home + slot]]


def slot_pick(code, plan, incoming, model_count):
    slots = CAP // DEVICES
    return pl.pallas_call(
        functools.partial(slot_kernel, model_count),
        in_specs=[whole(pltpu.SMEM), whole(pltpu.SMEM), whole()],
        out_specs=[whole()] * DEVICES,
        out_shape=[jax.ShapeDtypeStruct((slots, CHUNK, TILE), BF16)] * DEVICES,
        interpret=INTERPRET,
        compiler_params=params(8 * 2**20),
        name="slot_pick",
        cost_estimate=cost(2**21, 2**22),
    )(code, plan, incoming)


def total(value):
    return jnp.sum(jnp.sum(value, axis=0, keepdims=True), axis=1, keepdims=True)


def unpack(stack_ref, stat_ref):
    row_ids, column_ids = iota((TILE, TILE), 0), iota((TILE, TILE), 1)
    last_row = row_ids == TILE - 1
    for index, (row, column) in enumerate(ABOVE):
        value = stack_ref[rows_of(index)]
        stat_ref[rows_of(row), rows_of(column)] = value
        stat_ref[rows_of(column), rows_of(row)] = value.T
    shared, third, fourth = [stack_ref[rows_of(index)] for index in (6, 7, 8)]
    mirrored = shared.T
    diagonal = jnp.where(column_ids == TILE - 1, fourth[TILE - 1 :, :1], third[TILE - 1 :])
    stat_ref[rows_of(0), rows_of(0)] = jnp.where(column_ids >= row_ids, shared, mirrored)
    stat_ref[rows_of(1), rows_of(1)] = jnp.where(
        row_ids == column_ids, diagonal, jnp.where(column_ids < row_ids, shared, mirrored)
    )
    stat_ref[rows_of(2), rows_of(2)] = jnp.where(last_row, third.T, third)
    stat_ref[rows_of(3), rows_of(3)] = jnp.where(last_row, fourth.T, fourth)


def roots_of(data_count, stack_ref, stat_ref, pair_ref):
    stats = range(stack_ref.shape[0])
    on_diagonal = iota((BLOCK, BLOCK), 0) == iota((BLOCK, BLOCK), 1)
    scales, first, small = [], [], []
    for k in stats:
        unpack(stack_ref.at[k], stat_ref.at[k])
        statistic = stat_ref[k] * (1.0 / data_count)
        diagonal_mean = total(jnp.where(on_diagonal, statistic, 0.0)) * (1.0 / BLOCK)
        damped = statistic + jnp.where(on_diagonal, 0.1 * diagonal_mean, 0.0)
        mean_square = total(damped * damped) * (1.0 / BLOCK**2)
        norm_scale = BLOCK * jnp.sqrt(mean_square + 1e-06)
        scales.append(lax.rsqrt(jnp.sqrt(norm_scale)))
        first.append(damped * (1.0 / norm_scale))
        small.append(first[k].astype(BF16))
    square = [dot(small[k], small[k]) for k in stats]
    part = [(square[k] * 0.0625 - 0.625 * first[k]).astype(BF16) for k in stats]
    twice = [1.5625 * first[k] + dot(part[k], small[k]) for k in stats]
    for k in stats:
        pair_ref[k, :BLOCK] = part[k]
        pair_ref[k, BLOCK:] = twice[k].astype(BF16)
    both = [dot(pair_ref[k], pair_ref[k, BLOCK:]) for k in stats]
    second = [1.5625 * twice[k] + both[k][:BLOCK] for k in stats]
    pair = [
        (both[k][BLOCK:] * 0.0625 - 0.3125 * (first[k] + second[k])).astype(BF16) for k in stats
    ]
    small = [second[k].astype(BF16) for k in stats]
    square = [dot(small[k], small[k]) for k in stats]
    part = [(square[k] * 0.0625 - 0.625 * second[k]).astype(BF16) for k in stats]
    twice = [1.5625 * second[k] + dot(part[k], small[k]) for k in stats]
    third = [1.5625 * twice[k] + dot(part[k], twice[k].astype(BF16)) for k in stats]
    result = []
    for k in stats:
        rest = 1.25 * pair[k].astype(F32) - 0.390625 * third[k]
        rest = rest - 0.25 * dot(pair[k], third[k].astype(BF16))
        result.append((rest * scales[k], 1.953125 * scales[k]))
    return result, on_diagonal


def home_kernel(data_count, model_count, code_ref, *refs):
    sources, row_refs = refs[:DEVICES], refs[DEVICES : 2 * DEVICES]
    rows_ref, stack_ref, stat_ref, pair_ref = refs[2 * DEVICES :]
    device, _ = position(code_ref, model_count)
    row_ids = iota((BLOCK, BLOCK), 0)
    spare = (row_ids % ROWS == 1) & (iota((BLOCK, BLOCK), 1) == row_ids - 1)
    for bits, ref in zip(PARTNERS, sources):
        start = pl.multiple_of((device ^ bits) * CHUNK, 16)
        for stat in range(2):
            stack_ref[stat, pl.ds(start, CHUNK)] = ref[stat].astype(F32)
    roots, on_diagonal = roots_of(data_count, stack_ref, stat_ref, pair_ref)
    for stat, (rest, identity_part) in enumerate(roots):
        rest_mean = total(jnp.where(on_diagonal, rest, 0.0)) * (1.0 / BLOCK)
        center = (identity_part + rest_mean).astype(BF16).astype(F32)
        rest = rest + jnp.where(on_diagonal, identity_part - center, 0.0)
        sent = jnp.where(spare, center, rest).astype(BF16)
        for home in range(DEVICES):
            rows_ref[home] = sent[home * ROWS : (home + 1) * ROWS]
        for bits, row_ref in zip(PARTNERS, row_refs):
            row_ref[stat] = rows_ref[device ^ bits]


def home_roots(code, sources, data_count, model_count):
    return pl.pallas_call(
        functools.partial(home_kernel, data_count, model_count),
        in_specs=[whole(pltpu.SMEM)] + [whole()] * DEVICES,
        out_specs=[whole()] * DEVICES,
        out_shape=[jax.ShapeDtypeStruct((2, ROWS, BLOCK), BF16)] * DEVICES,
        scratch_shapes=[
            pltpu.VMEM((DEVICES, ROWS, BLOCK), BF16),
            pltpu.VMEM((2, PACKED_ROWS, TILE), F32),
            pltpu.VMEM((2, BLOCK, BLOCK), F32),
            pltpu.VMEM((2, 2 * BLOCK, BLOCK), BF16),
        ],
        interpret=INTERPRET,
        compiler_params=params(),
        name="home_roots",
        cost_estimate=cost(2 * 8 * 2 * BLOCK**3, 2**22),
    )(code, *sources)


def owner_kernel(
    data_count,
    model_count,
    code_ref,
    plan_ref,
    *refs,
):
    sources = refs[:DEVICES]
    out_ref, stack_ref, stat_ref, pair_ref, root_ref, sems = refs[DEVICES:]
    device, _ = position(code_ref, model_count)
    slots = out_ref.shape[0]
    for bits, ref in zip(PARTNERS, sources):
        start = pl.multiple_of((device ^ bits) * CHUNK, 16)
        for slot in range(slots):
            stack_ref[slot, pl.ds(start, CHUNK)] = ref[slot].astype(F32)
    roots, on_diagonal = roots_of(data_count, stack_ref, stat_ref, pair_ref)
    for slot, (rest, identity_part) in enumerate(roots):
        keep = slots * device + slot < plan_ref[CAP]
        root = rest + jnp.where(on_diagonal, identity_part, 0.0)
        root_ref[slot] = jnp.where(keep, root, 0.0)
        pltpu.make_async_copy(root_ref.at[slot], out_ref.at[slot], sems.at[slot]).start()
    for slot in range(slots):
        pltpu.make_async_copy(root_ref.at[slot], out_ref.at[slot], sems.at[slot]).wait()


def owner_roots(code, plan, sources, data_count, model_count):
    slots = sources[0].shape[0]
    return pl.pallas_call(
        functools.partial(owner_kernel, data_count, model_count),
        in_specs=[whole(pltpu.SMEM), whole(pltpu.SMEM)] + [whole()] * DEVICES,
        out_specs=whole(pltpu.HBM),
        out_shape=jax.ShapeDtypeStruct((slots, BLOCK, BLOCK), F32),
        scratch_shapes=[
            pltpu.VMEM((slots, PACKED_ROWS, TILE), F32),
            pltpu.VMEM((slots, BLOCK, BLOCK), F32),
            pltpu.VMEM((slots, 2 * BLOCK, BLOCK), BF16),
            pltpu.VMEM((slots, BLOCK, BLOCK), F32),
            pltpu.SemaphoreType.DMA((slots,)),
        ],
        interpret=INTERPRET,
        compiler_params=params(40 * 2**20),
        name="owner_roots",
        cost_estimate=cost(3 * 8 * 2 * BLOCK**3, 2**22),
    )(code, plan, *sources)


def finish_kernel(model_count, code_ref, *refs):
    out_ref = refs[-1]
    device, _ = position(code_ref, model_count)
    first = device * ROWS
    row_ids = iota((ROWS, BLOCK), 0)
    column_ids = iota((ROWS, BLOCK), 1) - first
    spare = (row_ids == 1) & (column_ids == 0)
    mirror = (row_ids == 0) & (column_ids == 1)
    on_diagonal = row_ids == column_ids
    for bits, ref in zip(PARTNERS, refs[:-1]):
        home = device ^ bits
        for stat in range(2):
            value = ref[stat].astype(F32)
            center = total(jnp.where(spare[:8], value[:8], 0.0))
            mirrored = total(jnp.where(mirror[:8], value[:8], 0.0))
            value = jnp.where(spare, mirrored, value)
            out_ref[2 * home + stat] = value + jnp.where(on_diagonal, center, 0.0)


def finish_rows(code, rows, model_count):
    return pl.pallas_call(
        functools.partial(finish_kernel, model_count),
        in_specs=[whole(pltpu.SMEM)] + [whole()] * DEVICES,
        out_specs=whole(),
        out_shape=jax.ShapeDtypeStruct((2 * DEVICES, ROWS, BLOCK), F32),
        interpret=INTERPRET,
        compiler_params=params(),
        name="finish_rows",
        cost_estimate=cost(2**21, 2**22),
    )(code, *rows)


def exchange(value, bits, data_count):
    return lax.ppermute(value, "dp", [(d, d ^ bits) for d in range(data_count)])


def exchange_all(values, data_count):
    return [values[0]] + [
        exchange(value, bits, data_count) for value, bits in zip(values[1:], PARTNERS[1:])
    ]


def program(gradients, owner_table):
    data_count = lax.axis_size("dp")
    model_count = lax.axis_size("mp")
    row_blocks = gradients.shape[1] // BLOCK
    blocks = gradients[0].reshape(row_blocks, BLOCK, BLOCK)
    code = (lax.axis_index("dp") * model_count + lax.axis_index("mp")).reshape(1)

    sources = []
    gram_code = code
    half = row_blocks // 2
    for group, cut in enumerate(CUTS):
        own, away = gram_blocks(blocks, gram_code, model_count, group * half, half, cut)
        if group == 0:
            gram_code, away = lax.optimization_barrier((gram_code, away))
        got = exchange(away, 1, data_count)
        for part, rows in enumerate((slice(0, cut), slice(cut, CHUNK))):
            first = own[:2, :, rows].astype(F32) + got[:2, :, rows].astype(F32)
            step = exchange(first.astype(BF16), FIRST_BITS[part], data_count)
            second = own[3:, :, rows].astype(F32) + got[3:, :, rows].astype(F32)
            second = second + step[1:].astype(F32)
            last = exchange(second.astype(BF16), SECOND_BITS[part], data_count)
            third = own[2, :, rows].astype(F32) + got[2, :, rows].astype(F32)
            sources += [third + step[0].astype(F32), last]

    plan = make_plan(code, owner_table, model_count)
    outgoing, *home = sum_and_send(code, plan, sources, model_count)
    incoming = lax.all_to_all(outgoing, "mp", split_axis=0, concat_axis=0, tiled=True)

    rows = list(home_roots(code, exchange_all(home, data_count), data_count, model_count))
    incoming, rows[0] = lax.optimization_barrier((incoming, rows[0]))
    rows = exchange_all(rows, data_count)
    slab_roots = finish_rows(code, rows, model_count)

    slots = slot_pick(code, plan, incoming, model_count)
    stacked = exchange_all(slots, data_count)
    root_stacks = owner_roots(code, plan, stacked, data_count, model_count)
    return (root_stacks[None], slab_roots)


def solution(mesh):
    placed = (P("dp", None, "mp"), P())
    return jax.shard_map(
        program,
        mesh=mesh,
        in_specs=placed,
        out_specs=(P("mp", "dp", None, None), P(None, "dp", "mp")),
        check_vma=False,
    )
```

```python
import functools

import jax
import jax.numpy as jnp
from jax import lax
from jax.experimental import pallas as pl
from jax.experimental.pallas import tpu as pltpu
from jax.sharding import PartitionSpec as P


CAP = 24
BLOCK = 512
TILE = 128
DEVICES = 8
ABOVE = [(0, 1), (0, 2), (0, 3), (1, 2), (1, 3), (2, 3)]
PACKED_ROWS = 9 * TILE
CHUNK = PACKED_ROWS // DEVICES
CUTS = (80, 64)
PARTNERS = (0, 4, 5, 6, 2, 7, 3, 1)
ROWS = BLOCK // DEVICES
ORDERS = ((1, 2, 0, 3), (3, 2, 0, 1))
FIRST_BITS = (2, 6)
SECOND_BITS = (6, 2)
VMEM_LIMIT = 24 * 2**20
INTERPRET = False
F32 = jnp.float32
BF16 = jnp.bfloat16


def rows_of(block):
    return slice(block * TILE, (block + 1) * TILE)


def dot(first, second, dims=((1,), (0,))):
    return lax.dot_general(first, second, (dims, ((), ())), preferred_element_type=F32)


def iota(shape, axis):
    return lax.broadcasted_iota(jnp.int32, shape, axis)


def whole(memory_space=pltpu.VMEM):
    return pl.BlockSpec(memory_space=memory_space)


def params(limit=VMEM_LIMIT):
    return pltpu.CompilerParams(vmem_limit_bytes=limit)


def position(code_ref, model_count):
    return code_ref[0] // model_count, code_ref[0] % model_count


def cost(flops, moved):
    return pl.CostEstimate(flops=int(flops), bytes_accessed=int(moved), transcendentals=0)


def gram_step(code_ref, model_count, cut, block, own_ref, away_ref, stack_ref):
    half = BLOCK // 2
    device, _ = position(code_ref, model_count)
    core = device & 1
    along = device >> 1
    row_ids, column_ids = iota((TILE, TILE), 0), iota((TILE, TILE), 1)
    last_row = row_ids == TILE - 1
    for side in range(2):
        dims = ((1,), (1,)) if side == 0 else ((0,), (0,))
        low = block[:half] if side == 0 else block[:, :half]
        high = block[half:] if side == 0 else block[:, half:]
        right = dot(block, high, dims)
        corner = dot(low, low, dims)

        def tile(row, column):
            if column >= 2:
                return right[rows_of(row), rows_of(column - 2)]
            return corner[rows_of(row), rows_of(column)]

        tiles = [tile(row, column) for row, column in ABOVE]
        inner = tile(1, 1)
        diagonal = jnp.sum(jnp.where(row_ids == column_ids, inner, 0.0), axis=0, keepdims=True)
        corner_end = inner[TILE - 1 :, TILE - 1 :]
        tiles.append(jnp.where(column_ids >= row_ids, tile(0, 0), inner))
        tiles.append(jnp.where(last_row & (column_ids < TILE - 1), diagonal, tile(2, 2)))
        tiles.append(jnp.where(last_row & (column_ids == 0), corner_end, tile(3, 3)))
        for index, value in enumerate(tiles):
            stack_ref[rows_of(index)] = value.astype(BF16)
        for chip in range(4):
            offset = chip ^ along
            for part, (start, stop) in enumerate(((0, cut), (cut, CHUNK))):
                place = jnp.int32(0)
                for spot, value in enumerate(ORDERS[part]):
                    place = jnp.where(offset == value, spot, place)
                base = 2 * chip * CHUNK
                even = stack_ref[base + start : base + stop]
                odd = stack_ref[base + CHUNK + start : base + CHUNK + stop]
                own_ref[place, side, start:stop] = jnp.where(core == 0, even, odd)
                away_ref[place, side, start:stop] = jnp.where(core == 0, odd, even)


def gram_kernel(model_count, cut, code_ref, block_ref, own_ref, away_ref, stack_ref):
    gram_step(code_ref, model_count, cut, block_ref[0], own_ref, away_ref, stack_ref)


def gram_blocks(blocks, code, model_count, first, count, cut):
    shape = jax.ShapeDtypeStruct((4, 2 * count, CHUNK, TILE), BF16)
    out_spec = pl.BlockSpec((4, 2, CHUNK, TILE), lambda step, code_ref: (0, step, 0, 0))
    in_spec = pl.BlockSpec((1, BLOCK, BLOCK), lambda step, code_ref: (first + step, 0, 0))
    return pl.pallas_call(
        functools.partial(gram_kernel, model_count, cut),
        out_shape=(shape, shape),
        grid_spec=pltpu.PrefetchScalarGridSpec(
            num_scalar_prefetch=1,
            grid=(count,),
            in_specs=[in_spec],
            out_specs=[out_spec, out_spec],
            scratch_shapes=[pltpu.VMEM((PACKED_ROWS, TILE), BF16)],
        ),
        interpret=INTERPRET,
        compiler_params=params(),
        cost_estimate=cost(3 * count * BLOCK**3, count * 5 * 2**18),
    )(code, blocks)


def plan_kernel(model_count, code_ref, table_ref, plan_ref):
    _, model = position(code_ref, model_count)
    for entry in range(plan_ref.shape[0]):
        plan_ref[entry] = 0
    per_slab = table_ref.shape[0] // model_count
    for stat in range(per_slab):
        plan_ref[CAP + 1 + table_ref[model * per_slab + stat]] = stat

    def slab_step(slab, count):
        named = jnp.int32(0)
        for stat in range(per_slab):
            named = named | jnp.where(table_ref[slab * per_slab + stat] == model, 1, 0)

        @pl.when(named > 0)
        def _():
            plan_ref[count] = slab

        return count + named

    plan_ref[CAP] = lax.fori_loop(0, model_count, slab_step, jnp.int32(0))


def make_plan(code, owner_table, model_count):
    return pl.pallas_call(
        functools.partial(plan_kernel, model_count),
        in_specs=[whole(pltpu.SMEM), whole(pltpu.SMEM)],
        out_specs=whole(pltpu.SMEM),
        out_shape=jax.ShapeDtypeStruct((CAP + 1 + model_count,), jnp.int32),
        interpret=INTERPRET,
        compiler_params=params(2**20),
        name="make_plan",
        cost_estimate=cost(2**22, 2**12),
    )(code, owner_table)


def sum_kernel(model_count, code_ref, plan_ref, *refs):
    sources = refs[:8]
    outgoing_ref, *home_refs = refs[8 : 9 + DEVICES]
    (mine_ref,) = refs[9 + DEVICES :]
    device, _ = position(code_ref, model_count)
    base = 0
    for group, cut in enumerate(CUTS):
        for part, (start, stop) in enumerate(((0, cut), (cut, CHUNK))):
            partial_ref, last_ref = sources[4 * group + 2 * part : 4 * group + 2 * part + 2]
            value = partial_ref[...] + last_ref[0].astype(F32)
            mine_ref[base : base + value.shape[0], start:stop] = value.astype(BF16)
        base += value.shape[0]
    for owner in range(model_count):
        outgoing_ref[owner] = mine_ref[plan_ref[CAP + 1 + owner]]
    for bits, home_ref in zip(PARTNERS, home_refs):
        home_ref[...] = mine_ref[pl.ds(2 * (device ^ bits), 2)]


def sum_and_send(code, plan, sources, model_count):
    home = jax.ShapeDtypeStruct((2, CHUNK, TILE), BF16)
    return pl.pallas_call(
        functools.partial(sum_kernel, model_count),
        in_specs=[whole(pltpu.SMEM), whole(pltpu.SMEM)] + [whole()] * 8,
        out_specs=[whole()] * (1 + DEVICES),
        out_shape=[jax.ShapeDtypeStruct((model_count, CHUNK, TILE), BF16)] + [home] * DEVICES,
        scratch_shapes=[
            pltpu.VMEM((2 * DEVICES, CHUNK, TILE), BF16),
        ],
        interpret=INTERPRET,
        compiler_params=params(),
        name="sum_and_send",
        cost_estimate=cost(2**21, 2**22),
    )(code, plan, *sources)


def slot_kernel(model_count, code_ref, plan_ref, source_ref, *slot_refs):
    device, _ = position(code_ref, model_count)
    slots = slot_refs[0].shape[0]
    for bits, slot_ref in zip(PARTNERS, slot_refs):
        home = device ^ bits
        for slot in range(slots):
            slot_ref[slot] = source_ref[plan_ref[slots * home + slot]]


def slot_pick(code, plan, incoming, model_count):
    slots = CAP // DEVICES
    return pl.pallas_call(
        functools.partial(slot_kernel, model_count),
        in_specs=[whole(pltpu.SMEM), whole(pltpu.SMEM), whole()],
        out_specs=[whole()] * DEVICES,
        out_shape=[jax.ShapeDtypeStruct((slots, CHUNK, TILE), BF16)] * DEVICES,
        interpret=INTERPRET,
        compiler_params=params(8 * 2**20),
        name="slot_pick",
        cost_estimate=cost(2**21, 2**22),
    )(code, plan, incoming)


def total(value):
    return jnp.sum(jnp.sum(value, axis=0, keepdims=True), axis=1, keepdims=True)


def unpack(stack_ref, stat_ref):
    row_ids, column_ids = iota((TILE, TILE), 0), iota((TILE, TILE), 1)
    last_row = row_ids == TILE - 1
    for index, (row, column) in enumerate(ABOVE):
        value = stack_ref[rows_of(index)]
        stat_ref[rows_of(row), rows_of(column)] = value
        stat_ref[rows_of(column), rows_of(row)] = value.T
    shared, third, fourth = [stack_ref[rows_of(index)] for index in (6, 7, 8)]
    mirrored = shared.T
    diagonal = jnp.where(column_ids == TILE - 1, fourth[TILE - 1 :, :1], third[TILE - 1 :])
    stat_ref[rows_of(0), rows_of(0)] = jnp.where(column_ids >= row_ids, shared, mirrored)
    stat_ref[rows_of(1), rows_of(1)] = jnp.where(
        row_ids == column_ids, diagonal, jnp.where(column_ids < row_ids, shared, mirrored)
    )
    stat_ref[rows_of(2), rows_of(2)] = jnp.where(last_row, third.T, third)
    stat_ref[rows_of(3), rows_of(3)] = jnp.where(last_row, fourth.T, fourth)


def roots_of(data_count, stack_ref, stat_ref, pair_ref):
    stats = range(stack_ref.shape[0])
    on_diagonal = iota((BLOCK, BLOCK), 0) == iota((BLOCK, BLOCK), 1)
    scales, first, small = [], [], []
    for k in stats:
        unpack(stack_ref.at[k], stat_ref.at[k])
        statistic = stat_ref[k] * (1.0 / data_count)
        diagonal_mean = total(jnp.where(on_diagonal, statistic, 0.0)) * (1.0 / BLOCK)
        damped = statistic + jnp.where(on_diagonal, 0.1 * diagonal_mean, 0.0)
        mean_square = total(damped * damped) * (1.0 / BLOCK**2)
        norm_scale = BLOCK * jnp.sqrt(mean_square + 1e-06)
        scales.append(lax.rsqrt(jnp.sqrt(norm_scale)))
        first.append(damped * (1.0 / norm_scale))
        small.append(first[k].astype(BF16))
    square = [dot(small[k], small[k]) for k in stats]
    part = [(square[k] * 0.0625 - 0.625 * first[k]).astype(BF16) for k in stats]
    twice = [1.5625 * first[k] + dot(part[k], small[k]) for k in stats]
    for k in stats:
        pair_ref[k, :BLOCK] = part[k]
        pair_ref[k, BLOCK:] = twice[k].astype(BF16)
    both = [dot(pair_ref[k], pair_ref[k, BLOCK:]) for k in stats]
    second = [1.5625 * twice[k] + both[k][:BLOCK] for k in stats]
    pair = [
        (both[k][BLOCK:] * 0.0625 - 0.3125 * (first[k] + second[k])).astype(BF16) for k in stats
    ]
    small = [second[k].astype(BF16) for k in stats]
    square = [dot(small[k], small[k]) for k in stats]
    part = [(square[k] * 0.0625 - 0.625 * second[k]).astype(BF16) for k in stats]
    twice = [1.5625 * second[k] + dot(part[k], small[k]) for k in stats]
    third = [1.5625 * twice[k] + dot(part[k], twice[k].astype(BF16)) for k in stats]
    result = []
    for k in stats:
        rest = 1.25 * pair[k].astype(F32) - 0.390625 * third[k]
        rest = rest - 0.25 * dot(pair[k], third[k].astype(BF16))
        result.append((rest * scales[k], 1.953125 * scales[k]))
    return result, on_diagonal


def home_kernel(data_count, model_count, code_ref, *refs):
    sources, row_refs = refs[:DEVICES], refs[DEVICES : 2 * DEVICES]
    rows_ref, stack_ref, stat_ref, pair_ref = refs[2 * DEVICES :]
    device, _ = position(code_ref, model_count)
    row_ids = iota((BLOCK, BLOCK), 0)
    spare = (row_ids % ROWS == 1) & (iota((BLOCK, BLOCK), 1) == row_ids - 1)
    for bits, ref in zip(PARTNERS, sources):
        start = pl.multiple_of((device ^ bits) * CHUNK, 16)
        for stat in range(2):
            stack_ref[stat, pl.ds(start, CHUNK)] = ref[stat].astype(F32)
    roots, on_diagonal = roots_of(data_count, stack_ref, stat_ref, pair_ref)
    for stat, (rest, identity_part) in enumerate(roots):
        rest_mean = total(jnp.where(on_diagonal, rest, 0.0)) * (1.0 / BLOCK)
        center = (identity_part + rest_mean).astype(BF16).astype(F32)
        rest = rest + jnp.where(on_diagonal, identity_part - center, 0.0)
        sent = jnp.where(spare, center, rest).astype(BF16)
        for home in range(DEVICES):
            rows_ref[home] = sent[home * ROWS : (home + 1) * ROWS]
        for bits, row_ref in zip(PARTNERS, row_refs):
            row_ref[stat] = rows_ref[device ^ bits]


def home_roots(code, sources, data_count, model_count):
    return pl.pallas_call(
        functools.partial(home_kernel, data_count, model_count),
        in_specs=[whole(pltpu.SMEM)] + [whole()] * DEVICES,
        out_specs=[whole()] * DEVICES,
        out_shape=[jax.ShapeDtypeStruct((2, ROWS, BLOCK), BF16)] * DEVICES,
        scratch_shapes=[
            pltpu.VMEM((DEVICES, ROWS, BLOCK), BF16),
            pltpu.VMEM((2, PACKED_ROWS, TILE), F32),
            pltpu.VMEM((2, BLOCK, BLOCK), F32),
            pltpu.VMEM((2, 2 * BLOCK, BLOCK), BF16),
        ],
        interpret=INTERPRET,
        compiler_params=params(),
        name="home_roots",
        cost_estimate=cost(2 * 8 * 2 * BLOCK**3, 2**22),
    )(code, *sources)


def owner_kernel(
    data_count,
    model_count,
    code_ref,
    plan_ref,
    *refs,
):
    sources = refs[:DEVICES]
    out_ref, stack_ref, stat_ref, pair_ref, root_ref, sems = refs[DEVICES:]
    device, _ = position(code_ref, model_count)
    slots = out_ref.shape[0]
    for bits, ref in zip(PARTNERS, sources):
        start = pl.multiple_of((device ^ bits) * CHUNK, 16)
        for slot in range(slots):
            stack_ref[slot, pl.ds(start, CHUNK)] = ref[slot].astype(F32)
    roots, on_diagonal = roots_of(data_count, stack_ref, stat_ref, pair_ref)
    for slot, (rest, identity_part) in enumerate(roots):
        keep = slots * device + slot < plan_ref[CAP]
        root = rest + jnp.where(on_diagonal, identity_part, 0.0)
        root_ref[slot] = jnp.where(keep, root, 0.0)
        pltpu.make_async_copy(root_ref.at[slot], out_ref.at[slot], sems.at[slot]).start()
    for slot in range(slots):
        pltpu.make_async_copy(root_ref.at[slot], out_ref.at[slot], sems.at[slot]).wait()


def owner_roots(code, plan, sources, data_count, model_count):
    slots = sources[0].shape[0]
    return pl.pallas_call(
        functools.partial(owner_kernel, data_count, model_count),
        in_specs=[whole(pltpu.SMEM), whole(pltpu.SMEM)] + [whole()] * DEVICES,
        out_specs=whole(pltpu.HBM),
        out_shape=jax.ShapeDtypeStruct((slots, BLOCK, BLOCK), F32),
        scratch_shapes=[
            pltpu.VMEM((slots, PACKED_ROWS, TILE), F32),
            pltpu.VMEM((slots, BLOCK, BLOCK), F32),
            pltpu.VMEM((slots, 2 * BLOCK, BLOCK), BF16),
            pltpu.VMEM((slots, BLOCK, BLOCK), F32),
            pltpu.SemaphoreType.DMA((slots,)),
        ],
        interpret=INTERPRET,
        compiler_params=params(40 * 2**20),
        name="owner_roots",
        cost_estimate=cost(3 * 8 * 2 * BLOCK**3, 2**22),
    )(code, plan, *sources)


def finish_kernel(model_count, code_ref, *refs):
    out_ref = refs[-1]
    device, _ = position(code_ref, model_count)
    first = device * ROWS
    row_ids = iota((ROWS, BLOCK), 0)
    column_ids = iota((ROWS, BLOCK), 1) - first
    spare = (row_ids == 1) & (column_ids == 0)
    mirror = (row_ids == 0) & (column_ids == 1)
    on_diagonal = row_ids == column_ids
    for bits, ref in zip(PARTNERS, refs[:-1]):
        home = device ^ bits
        for stat in range(2):
            value = ref[stat].astype(F32)
            center = total(jnp.where(spare[:8], value[:8], 0.0))
            mirrored = total(jnp.where(mirror[:8], value[:8], 0.0))
            value = jnp.where(spare, mirrored, value)
            out_ref[2 * home + stat] = value + jnp.where(on_diagonal, center, 0.0)


def finish_rows(code, rows, model_count):
    return pl.pallas_call(
        functools.partial(finish_kernel, model_count),
        in_specs=[whole(pltpu.SMEM)] + [whole()] * DEVICES,
        out_specs=whole(),
        out_shape=jax.ShapeDtypeStruct((2 * DEVICES, ROWS, BLOCK), F32),
        interpret=INTERPRET,
        compiler_params=params(),
        name="finish_rows",
        cost_estimate=cost(2**21, 2**22),
    )(code, *rows)


def exchange(value, bits, data_count):
    return lax.ppermute(value, "dp", [(d, d ^ bits) for d in range(data_count)])


def exchange_all(values, data_count):
    return [values[0]] + [
        exchange(value, bits, data_count) for value, bits in zip(values[1:], PARTNERS[1:])
    ]


def program(gradients, owner_table):
    data_count = lax.axis_size("dp")
    model_count = lax.axis_size("mp")
    row_blocks = gradients.shape[1] // BLOCK
    blocks = gradients[0].reshape(row_blocks, BLOCK, BLOCK)
    code = (lax.axis_index("dp") * model_count + lax.axis_index("mp")).reshape(1)

    sources = []
    gram_code = code
    half = row_blocks // 2
    for group, cut in enumerate(CUTS):
        own, away = gram_blocks(blocks, gram_code, model_count, group * half, half, cut)
        if group == 0:
            gram_code, away = lax.optimization_barrier((gram_code, away))
        got = exchange(away, 1, data_count)
        for part, rows in enumerate((slice(0, cut), slice(cut, CHUNK))):
            first = own[:2, :, rows].astype(F32) + got[:2, :, rows].astype(F32)
            step = exchange(first.astype(BF16), FIRST_BITS[part], data_count)
            second = own[3:, :, rows].astype(F32) + got[3:, :, rows].astype(F32)
            second = second + step[1:].astype(F32)
            last = exchange(second.astype(BF16), SECOND_BITS[part], data_count)
            third = own[2, :, rows].astype(F32) + got[2, :, rows].astype(F32)
            sources += [third + step[0].astype(F32), last]

    plan = make_plan(code, owner_table, model_count)
    outgoing, *home = sum_and_send(code, plan, sources, model_count)
    incoming = lax.all_to_all(outgoing, "mp", split_axis=0, concat_axis=0, tiled=True)

    rows = list(home_roots(code, exchange_all(home, data_count), data_count, model_count))
    incoming, rows[0] = lax.optimization_barrier((incoming, rows[0]))
    rows = exchange_all(rows, data_count)
    slab_roots = finish_rows(code, rows, model_count)

    slots = slot_pick(code, plan, incoming, model_count)
    stacked = exchange_all(slots, data_count)
    root_stacks = owner_roots(code, plan, stacked, data_count, model_count)
    return (root_stacks[None], slab_roots)


def solution(mesh):
    placed = (P("dp", None, "mp"), P())
    return jax.shard_map(
        program,
        mesh=mesh,
        in_specs=placed,
        out_specs=(P("mp", "dp", None, None), P(None, "dp", "mp")),
        check_vma=False,
    )
```
